512 devices in a mesh: leaf: 16 (over y_hi, x, core), ctx: 32 (over z, y_lo).
Axes of the slice: x: 4, y: 4 (y_hi: 2, y_lo: 2; y = y_hi * 2 + y_lo), z: 16, core: 2. Of those that a mesh axis runs over, the one named last changes fastest.
Arguments:
- queries: bfloat16 [65536, 4096], P(('leaf', 'ctx')), parts along dimension 0, may hold values from -6 to 6
- keys: bfloat16 [65536, 512], P(('leaf', 'ctx')), parts along dimension 0, may hold values from -6 to 6
- values: bfloat16 [65536, 512], P(('leaf', 'ctx')), parts along dimension 0, may hold values from -6 to 6
- grad_out: bfloat16 [65536, 4096], P(('leaf', 'ctx')), parts along dimension 0, may hold values from -6 to 6
- block_path: int32 [512, 4], P('leaf'), parts along dimension 0, may hold values from -1 to 31, as said below
- assistant: int32 [65536], P(('leaf', 'ctx')), parts along dimension 0, may hold values from 0 to 1, as said below
Outputs:
- attention: bfloat16 [65536, 4096], P(('leaf', 'ctx')), parts along dimension 0
- grad_queries: bfloat16 [65536, 4096], P(('leaf', 'ctx')), parts along dimension 0
- grad_keys: bfloat16 [65536, 512], P(('leaf', 'ctx')), parts along dimension 0
- grad_values: bfloat16 [65536, 512], P(('leaf', 'ctx')), parts along dimension 0
The draws below stay inside these ranges and needn't reach their ends.
There are 16 independent parts, one for each index of `leaf`. The reference program is written for one: setup_inputs(seed, part) draws one part's arguments, and reference() takes and returns one part's arrays. A program takes and returns all parts, laid end to end along the dimension named above; each array names one. Nothing has to cross between parts.
Inputs may be any that keep to these rules, and one draw needn't show every extreme that they name: `block_path`: blocks lie in depth-first order of the tree; every node spans one block; block 0 is the root at depth 0. Row b holds at depth e <= depth(b) the block of b's ancestor node at that depth (b itself at e = depth(b)) and -1 below. `assistant`: each block of 128 tokens holds one run of ones.
All inputs are finite; a program needn't handle non-finite values.
Results may differ from the reference program's by a relative error of at most 0.0091.
Values may be sent and summed in bfloat16 or wider, within the bound.
A program may use at most 128 MiB of HBM per device.

```python
import math
import jax
import jax.numpy as jnp
from jax import lax

TOK_DEV = 128
HQ = 32
KEY_HEADS = 4
HEAD_WIDTH = 128
HEADS_PER_KEY = 8
NBLK = 32
TREE_TOKENS = 4096


def tree_paths(key):
    block_keys = jax.random.split(jax.random.fold_in(key, 3), NBLK - 1)

    def advance(state, inputs):
        own_path, depth_now = state
        block_index, block_key = inputs
        highest = jnp.minimum(depth_now + 1, 3)
        depth_next = jax.random.randint(block_key, (), 1, highest + 1).astype(jnp.int32)
        tier_index = jnp.arange(4, dtype=jnp.int32)
        path_next = jnp.where(tier_index < depth_next, own_path, jnp.where(tier_index == depth_next, block_index, -1)).astype(jnp.int32)
        return ((path_next, depth_next), path_next)
    first_path = jnp.array([0, -1, -1, -1], dtype=jnp.int32)
    initial = (first_path, jnp.int32(0))
    _, rest_rows = lax.scan(advance, initial, (jnp.arange(1, NBLK, dtype=jnp.int32), block_keys))
    return jnp.concatenate([first_path[None, :], rest_rows], 0)


def draw_block_path(key, part):
    return tree_paths(key)


def draw_assistant(key, part):
    first_key, second_key = jax.random.split(jax.random.fold_in(key, 7))
    begin_at = jax.random.randint(first_key, (NBLK, 1), 0, TOK_DEV // 2)
    span_rows = jax.random.randint(second_key, (NBLK, 1), TOK_DEV // 4, TOK_DEV)
    offsets = jnp.arange(TOK_DEV)[None, :]
    inside = (offsets >= begin_at) & (offsets < begin_at + span_rows)
    return inside.astype(jnp.int32).reshape(-1)


def query_key_pair(key):
    base_key = jax.random.fold_in(key, 11)
    query_base, key_seed = jax.random.split(base_key, 2)
    query_draw = jnp.clip(jax.random.normal(query_base, (TREE_TOKENS, HQ * HEAD_WIDTH), jnp.float32), -6.0, 6.0)
    key_sample = jnp.clip(jax.random.normal(key_seed, (TREE_TOKENS, KEY_HEADS * HEAD_WIDTH), jnp.float32), -6.0, 6.0)
    return (query_draw, key_sample)


def draw_queries(key, part):
    return query_key_pair(key)[0].astype(jnp.bfloat16)


def draw_keys(key, part):
    return query_key_pair(key)[1].astype(jnp.bfloat16)


def level_of(rng, shape, cuts, least, largest):
    gain, own = 1.0, jax.random.fold_in(rng, 6)
    for dim, parts in cuts:
        steps = jnp.exp(jax.random.uniform(jax.random.fold_in(own, dim), (parts,), jnp.float32, least / len(cuts), largest / len(cuts)))
        gain = gain * jnp.repeat(steps, shape[dim] // parts).reshape([-1 if axis == dim else 1 for axis in range(len(shape))])
    return gain


def gaussian(key, dims, width, reach, pieces=(), kind=jnp.bfloat16):
    drawn = width * jax.random.normal(key, dims, jnp.float32)
    if pieces:
        drawn = drawn * level_of(key, dims, pieces, -0.22, 0.18)
    return jnp.clip(drawn, -reach, reach).astype(kind)


def setup_inputs(seed: int = 0, part: int = 0) -> dict:
    splits = jax.random.split(jax.random.key(seed), 7)
    part_keys = jax.random.split(jax.random.fold_in(splits[6], part), 7)
    queries = draw_queries(jax.random.fold_in(jax.random.fold_in(splits[6], part), 71), part)
    keys = draw_keys(jax.random.fold_in(jax.random.fold_in(splits[6], part), 71), part)
    values = gaussian(part_keys[2], (TREE_TOKENS, KEY_HEADS * HEAD_WIDTH), 1.0, 6.0, ((0, 32),))
    grad_out = gaussian(part_keys[3], (TREE_TOKENS, HQ * HEAD_WIDTH), 1.0, 6.0, ((0, 32),))
    block_path = draw_block_path(jax.random.fold_in(jax.random.fold_in(splits[6], part), 71), part)
    assistant = draw_assistant(jax.random.fold_in(jax.random.fold_in(splits[6], part), 71), part)
    return {"queries": queries, "keys": keys, "values": values, "grad_out": grad_out, "block_path": block_path, "assistant": assistant}


def attend_block(queries, grad_rows, slot_keys, slot_values, allowed):
    block_rows = queries.shape[0]
    head_cols = HEADS_PER_KEY * HEAD_WIDTH
    scaling = 1.0 / math.sqrt(HEAD_WIDTH)
    wide_mask = jnp.repeat(allowed, HEADS_PER_KEY, axis=0)
    attended_parts, query_parts, key_parts, value_parts = ([], [], [], [])
    for key_value_head in range(KEY_HEADS):
        query_matrix = queries[:, key_value_head * head_cols:(key_value_head + 1) * head_cols].reshape(block_rows * HEADS_PER_KEY, HEAD_WIDTH)
        grad_head = grad_rows[:, key_value_head * head_cols:(key_value_head + 1) * head_cols].reshape(block_rows * HEADS_PER_KEY, HEAD_WIDTH)
        key_cols = slot_keys[:, key_value_head * HEAD_WIDTH:(key_value_head + 1) * HEAD_WIDTH]
        value_cols = slot_values[:, key_value_head * HEAD_WIDTH:(key_value_head + 1) * HEAD_WIDTH]
        scores = jnp.dot(query_matrix, key_cols.T, preferred_element_type=jnp.float32) * scaling
        scores = jnp.where(wide_mask, scores, -jnp.inf)
        row_max = lax.optimization_barrier(jnp.max(scores, axis=1, keepdims=True))
        row_sum = lax.optimization_barrier(jnp.sum(jnp.exp(scores - row_max), axis=1, keepdims=True))
        weights = jnp.exp(scores - (row_max + jnp.log(row_sum)))
        rounded = weights.astype(jnp.bfloat16)
        attended = jnp.dot(rounded, value_cols, preferred_element_type=jnp.float32).astype(jnp.bfloat16)
        attended = lax.optimization_barrier(attended)
        row_delta = lax.optimization_barrier(jnp.sum(grad_head.astype(jnp.float32) * attended.astype(jnp.float32), axis=1, keepdims=True))
        grad_prob = jnp.dot(grad_head, value_cols.T, preferred_element_type=jnp.float32)
        grad_score = (weights * (grad_prob - row_delta)).astype(jnp.bfloat16)
        grad_query = (jnp.dot(grad_score, key_cols, preferred_element_type=jnp.float32) * scaling).astype(jnp.bfloat16)
        grad_key = jnp.dot(grad_score.T, query_matrix, preferred_element_type=jnp.float32) * scaling
        grad_value = jnp.dot(rounded.T, grad_head, preferred_element_type=jnp.float32)
        attended_parts.append(attended.reshape(block_rows, head_cols))
        query_parts.append(grad_query.reshape(block_rows, head_cols))
        key_parts.append(grad_key)
        value_parts.append(grad_value)
    return (jnp.concatenate(attended_parts, 1), jnp.concatenate(query_parts, 1), jnp.concatenate(key_parts, 1), jnp.concatenate(value_parts, 1))

def reference(queries, keys, values, grad_out, block_path, assistant):
    blocks = block_path.shape[0]
    block_rows = queries.shape[0] // blocks
    kv_width = keys.shape[1]
    depths = lax.optimization_barrier(jnp.sum((block_path >= 0).astype(jnp.int32), axis=1)) - 1
    key_blocks = keys.reshape(blocks, block_rows, kv_width)
    value_blocks = values.reshape(blocks, block_rows, kv_width)
    query_blocks = queries.reshape(blocks, block_rows, queries.shape[1])
    grad_rows = grad_out * assistant[:, None].astype(jnp.bfloat16)
    grad_blocks = grad_rows.reshape(blocks, block_rows, grad_out.shape[1])
    causal = jnp.arange(block_rows)[:, None] >= jnp.arange(block_rows)[None, :]

    def one_block(carried, block_index):
        key_total, value_total = carried
        own_path = block_path[block_index]
        own_depth = depths[block_index]
        slot_blocks = jnp.stack([own_path[0], own_path[1], own_path[2], block_index]).astype(jnp.int32)
        seen_slots = jnp.stack([own_depth > 0, own_depth > 1, own_depth > 2])
        clipped = jnp.clip(slot_blocks, 0, blocks - 1)
        slot_keys = key_blocks[clipped].reshape(4 * block_rows, kv_width)
        slot_values = value_blocks[clipped].reshape(4 * block_rows, kv_width)
        full_slots = jnp.repeat(seen_slots, block_rows)
        allowed = jnp.concatenate([jnp.broadcast_to(full_slots[None, :], (block_rows, 3 * block_rows)), causal], 1)
        attended, grad_query, grad_key, grad_value = attend_block(query_blocks[block_index], grad_blocks[block_index], slot_keys, slot_values, allowed)
        key_total = key_total.at[clipped].add(grad_key.reshape(4, block_rows, kv_width))
        value_total = value_total.at[clipped].add(grad_value.reshape(4, block_rows, kv_width))
        return ((key_total, value_total), (attended, grad_query))
    blank = jnp.zeros((blocks, block_rows, kv_width), jnp.float32)
    (key_total, value_total), (attended, grad_query) = lax.scan(one_block, (blank, blank), jnp.arange(blocks, dtype=jnp.int32))
    return (attended.reshape(-1, queries.shape[1]), grad_query.reshape(-1, queries.shape[1]), key_total.reshape(-1, kv_width).astype(jnp.bfloat16), value_total.reshape(-1, kv_width).astype(jnp.bfloat16))
```

```python
import functools
import math

import jax
import jax.numpy as jnp
from jax import lax
from jax.experimental import pallas as pl
from jax.experimental.pallas import tpu as pltpu
from jax.sharding import PartitionSpec as P

KEY_HEADS = 4
WIDTH = 128
GROUP = 8
ROWS = 128
NZ = 16
HALF = NZ // 2
PARTS = 2
CHUNK = ROWS // PARTS
CHUNKS = KEY_HEADS * 2 * PARTS
SCALE = 1.0 / math.sqrt(WIDTH)
EXP2_SCALE = SCALE * math.log2(math.e)
MASKED = -1e30


def place():
    me = lax.axis_index("ctx")
    return me, me // 2, lax.rem(me, 2)


def depth_of(paths, block):
    total = jnp.int32(-1)
    for e in range(4):
        total = total + (paths[block, e] >= 0).astype(jnp.int32)
    return total


def send(src, dst, send_sem, recv_sem, ctx):
    return pltpu.make_async_remote_copy(
        src_ref=src,
        dst_ref=dst,
        send_sem=send_sem,
        recv_sem=recv_sem,
        device_id={"ctx": ctx},
        device_id_type=pl.DeviceIdType.MESH,
    )


def greet(peers):
    barrier = pltpu.get_barrier_semaphore()
    for peer in peers:
        pl.semaphore_signal(
            barrier, inc=1, device_id={"ctx": peer}, device_id_type=pl.DeviceIdType.MESH
        )
    pl.semaphore_wait(barrier, len(peers))


def spread_kernel(
    paths, keys, values, slots, own, mate, root, seen, out,
    mate_send, mate_recv, root_send, root_recv, root_send2, chain_send, chain_recv,
):
    me, z, y = place()
    up = lax.rem(z + 1, NZ) * 2 + y
    down = lax.rem(z + NZ - 1, NZ) * 2 + y
    partner = z * 2 + 1 - y
    for h in range(KEY_HEADS):
        for t, ref in enumerate((keys, values)):
            first = (h * 2 + t) * PARTS
            own[first : first + PARTS] = ref[:, h * WIDTH : (h + 1) * WIDTH].reshape(
                PARTS, CHUNK, WIDTH
            )
    greet((up, down, partner))

    def to_mate(i):
        return send(own.at[i], mate.at[i], mate_send.at[i], mate_recv.at[i], partner)

    def to_next(i):
        return send(out.at[i], seen.at[i], chain_send.at[i], chain_recv.at[i], up)

    onward = jnp.where(z < HALF, up, down)

    def root_on(i):
        return send(root.at[i], root.at[i], root_send.at[i], root_recv.at[i], onward)

    def root_back(i):
        return send(root.at[i], root.at[i], root_send2.at[i], root_recv.at[i], down)

    @pl.loop(0, CHUNKS)
    def _(i):
        to_mate(i).start()

    d_own = depth_of(paths, me)
    d_mate = depth_of(paths, partner)

    def chain():
        @pl.loop(0, CHUNKS)
        def _(i):
            to_mate(i).wait_recv()
            mine = own[i]
            theirs = mate[i]

            @pl.when(z == 0)
            def _():
                seen[i, 0] = mine
                seen[i, 1] = mine

            @pl.when(z > 0)
            def _():
                to_next(i).wait_recv()

            for e in (1, 2):
                before = seen[i, e - 1]
                mate_hit = d_mate == e
                own_hit = d_own == e
                take_mate = mate_hit & ((y == 0) | (d_own != e))
                out[i, e - 1] = lax.select(
                    take_mate, theirs, lax.select(own_hit, mine, before)
                )
                slots[i, e] = lax.select(mate_hit & (y == 1), theirs, before)

            @pl.when(z < NZ - 1)
            def _():
                to_next(i).start()

    def roots():
        @pl.loop(0, CHUNKS)
        def _(i):
            @pl.when(z == 0)
            def _():
                root[i] = lax.select(y == 0, own[i], mate[i])

            @pl.when(z > 0)
            def _():
                root_on(i).wait_recv()

            slots[i, 0] = root[i]

            @pl.when((z != HALF - 1) & (z != HALF))
            def _():
                root_on(i).start()

            @pl.when(z == 0)
            def _():
                root_back(i).start()

    @pl.when(z >= HALF)
    def _():
        roots()

    chain()

    @pl.when(z < HALF)
    def _():
        roots()

    @pl.loop(0, CHUNKS)
    def _(i):
        to_mate(i).wait_send()

        @pl.when(z < NZ - 1)
        def _():
            to_next(i).wait_send()

        @pl.when((z != HALF - 1) & (z != HALF))
        def _():
            root_on(i).wait_send()

        @pl.when(z == 0)
        def _():
            root_back(i).wait_send()


def attend_kernel(
    paths, assistant, queries, grad_out, keys, values, far, attention, grad_queries, grads,
    bias, live,
):
    me, _, _ = place()
    cols = 2 * ROWS

    @pl.when(pl.program_id(0) == 0)
    def _():
        depth = depth_of(paths, me)
        for e in range(3):
            bias[e * ROWS : (e + 1) * ROWS] = jnp.full(
                (ROWS, cols), jnp.where(e < depth, 0.0, MASKED), jnp.float32
            )
        key_at = lax.broadcasted_iota(jnp.int32, (ROWS, cols), 0)
        row_at = lax.broadcasted_iota(jnp.int32, (ROWS, cols), 1)
        row_at = jnp.where(row_at >= ROWS, row_at - ROWS, row_at)
        bias[3 * ROWS :] = jnp.where(key_at <= row_at, 0.0, MASKED)
        r = lax.broadcasted_iota(jnp.int32, (ROWS, ROWS), 0)
        c = lax.broadcasted_iota(jnp.int32, (ROWS, ROWS), 1)
        spread = jnp.where(r == c, assistant[...].astype(jnp.float32), 0.0)
        live[...] = jnp.broadcast_to(
            jnp.sum(spread, axis=1, keepdims=True), (ROWS, ROWS)
        ).astype(jnp.bfloat16)

    far_keys = [far[0:PARTS, e].reshape(ROWS, WIDTH) for e in range(3)]
    far_values = [far[PARTS : 2 * PARTS, e].reshape(ROWS, WIDTH) for e in range(3)]
    k4 = jnp.concatenate(far_keys + [keys[...]], 0)
    v4 = jnp.concatenate(far_values + [values[...]], 0)
    k4t = k4.T
    v4t = v4.T
    dims = (((1,), (1,)), ((), ()))
    for pair in range(GROUP // 2):
        at = [slice((2 * pair + j) * WIDTH, (2 * pair + j + 1) * WIDTH) for j in range(2)]
        q2 = jnp.concatenate([queries[:, s] for s in at], 0)
        g2 = jnp.concatenate([grad_out[:, s] * live[...] for s in at], 0)
        s = lax.dot_general(k4, q2, dims, preferred_element_type=jnp.float32) + bias[...]
        top = jnp.max(s, axis=0, keepdims=True)
        p = jnp.exp2((s - top) * EXP2_SCALE)
        w = p * (1.0 / jnp.sum(p, axis=0, keepdims=True))
        wb = w.astype(jnp.bfloat16)
        out_t = jnp.dot(v4t, wb, preferred_element_type=jnp.float32)
        dp = lax.dot_general(v4, g2, dims, preferred_element_type=jnp.float32)
        out_t = out_t.astype(jnp.bfloat16)
        delta = jnp.sum(
            g2.T.astype(jnp.float32) * out_t.astype(jnp.float32), axis=0, keepdims=True
        )
        ds = (w * (dp - delta)).astype(jnp.bfloat16)
        gq_t = jnp.dot(k4t, ds, preferred_element_type=jnp.float32) * SCALE
        out = out_t.T
        gq = gq_t.astype(jnp.bfloat16).T
        for j in range(2):
            attention[:, at[j]] = out[j * ROWS : (j + 1) * ROWS]
            grad_queries[:, at[j]] = gq[j * ROWS : (j + 1) * ROWS]
        dk = jnp.dot(ds, q2, preferred_element_type=jnp.float32)
        dv = jnp.dot(wb, g2, preferred_element_type=jnp.float32)
        for t, d in enumerate((dk * SCALE, dv)):
            for e in range(4):
                new = d[e * ROWS : (e + 1) * ROWS].reshape(PARTS, CHUNK, WIDTH)
                here = slice(t * PARTS, (t + 1) * PARTS)
                if pair == 0:
                    grads[here, e] = new
                else:
                    grads[here, e] += new


def gather_kernel(
    paths, grads, grad_keys, grad_values,
    seen, out, total, root_in, root_last, root_out, rooted, to_x, from_x,
    chain_send, chain_recv, root_send, root_recv, last_recv, x_send, x_recv,
):
    me, z, y = place()
    up = lax.rem(z + 1, NZ) * 2 + y
    down = lax.rem(z + NZ - 1, NZ) * 2 + y
    partner = z * 2 + 1 - y
    greet((up, down, partner))
    d0 = depth_of(paths, z * 2)
    d1 = depth_of(paths, z * 2 + 1)
    late = (y == 1).astype(jnp.float32)
    early = 1.0 - late
    hit0 = [(d0 == e).astype(jnp.float32) for e in (1, 2)]
    hit1 = [(d1 == e).astype(jnp.float32) for e in (1, 2)]

    def to_next(i):
        return send(out.at[i], seen.at[i], chain_send.at[i], chain_recv.at[i], down)

    def to_mate(i):
        return send(to_x.at[i], from_x.at[i], x_send.at[i], x_recv.at[i], partner)

    onward = jnp.where(z < HALF, down, up)

    def root_on(i):
        return send(root_out.at[i], root_in.at[i], root_send.at[i], root_recv.at[i], onward)

    def root_end(i):
        return send(root_out.at[i], root_last.at[i], root_send.at[i], last_recv.at[i], onward)

    def chain():
        @pl.loop(0, CHUNKS)
        def _(i):
            @pl.when(z == NZ - 1)
            def _():
                seen[i] = jnp.zeros((2, CHUNK, WIDTH), jnp.bfloat16)

            @pl.when(z < NZ - 1)
            def _():
                to_next(i).wait_recv()

            taken0 = rooted[i]
            taken1 = jnp.zeros((CHUNK, WIDTH), jnp.float32)
            for e in (1, 2):
                before = seen[i, e - 1].astype(jnp.float32)
                mine = grads[i, e]
                taken1 = taken1 + hit1[e - 1] * before
                mid = (1.0 - hit1[e - 1]) * before + late * mine
                taken0 = taken0 + hit0[e - 1] * mid
                out[i, e - 1] = ((1.0 - hit0[e - 1]) * mid + early * mine).astype(jnp.bfloat16)

            @pl.when(z > 0)
            def _():
                to_next(i).start()

            to_x[i] = (early * taken1 + late * taken0).astype(jnp.bfloat16)
            to_mate(i).start()
            total[i] = grads[i, 3] + (early * taken0 + late * taken1)

    def roots():
        @pl.loop(0, CHUNKS)
        def _(i):
            rooted[i] = jnp.zeros((CHUNK, WIDTH), jnp.float32)

            @pl.when((z == HALF - 1) | (z == HALF))
            def _():
                root_out[i] = grads[i, 0].astype(jnp.bfloat16)

            @pl.when((z != HALF - 1) & (z != HALF))
            def _():
                root_on(i).wait_recv()
                root_out[i] = (grads[i, 0] + root_in[i].astype(jnp.float32)).astype(jnp.bfloat16)

            @pl.when(z == 0)
            def _():
                root_end(i).wait_recv()
                rooted[i] = (
                    grads[i, 0]
                    + root_in[i].astype(jnp.float32)
                    + root_last[i].astype(jnp.float32)
                )

            @pl.when((z > 0) & (z < NZ - 1))
            def _():
                root_on(i).start()

            @pl.when(z == NZ - 1)
            def _():
                root_end(i).start()

    @pl.when(z < NZ - 1)
    def _():
        roots()

    @pl.when(z == NZ - 1)
    def _():
        rooted[...] = jnp.zeros_like(rooted)

    chain()

    @pl.when(z == NZ - 1)
    def _():
        roots()

    @pl.loop(0, CHUNKS)
    def _(i):
        to_mate(i).wait_recv()
        total[i] += from_x[i].astype(jnp.float32)

    for h in range(KEY_HEADS):
        for t, ref in enumerate((grad_keys, grad_values)):
            first = (h * 2 + t) * PARTS
            ref[:, h * WIDTH : (h + 1) * WIDTH] = (
                total[first : first + PARTS].reshape(ROWS, WIDTH).astype(jnp.bfloat16)
            )

    @pl.loop(0, CHUNKS)
    def _(i):
        to_mate(i).wait_send()

        @pl.when(z > 0)
        def _():
            to_next(i).wait_send()
            root_on(i).wait_send()


def vmem():
    return pl.BlockSpec(memory_space=pltpu.VMEM)


def smem():
    return pl.BlockSpec(memory_space=pltpu.SMEM)


def on_device(queries, keys, values, grad_out, block_path, assistant):
    sems = pltpu.SemaphoreType.DMA((CHUNKS,))
    one = pltpu.VMEM((CHUNKS, CHUNK, WIDTH), jnp.bfloat16)
    two = pltpu.VMEM((CHUNKS, 2, CHUNK, WIDTH), jnp.bfloat16)
    wide = pltpu.VMEM((CHUNKS, CHUNK, WIDTH), jnp.float32)
    far = pl.pallas_call(
        spread_kernel,
        out_shape=jax.ShapeDtypeStruct((CHUNKS, 3, CHUNK, WIDTH), jnp.bfloat16),
        in_specs=[smem(), vmem(), vmem()],
        out_specs=vmem(),
        scratch_shapes=[one, one, one, two, two] + [sems] * 7,
        compiler_params=pltpu.CompilerParams(collective_id=0, has_side_effects=True),
        name="spread",
    )(block_path, keys, values)

    group = GROUP * WIDTH
    per = 2 * PARTS
    attention, grad_queries, grads = pl.pallas_call(
        attend_kernel,
        grid=(KEY_HEADS,),
        out_shape=(
            jax.ShapeDtypeStruct(queries.shape, jnp.bfloat16),
            jax.ShapeDtypeStruct(queries.shape, jnp.bfloat16),
            jax.ShapeDtypeStruct((CHUNKS, 4, CHUNK, WIDTH), jnp.float32),
        ),
        in_specs=[
            smem(),
            pl.BlockSpec((1, ROWS), lambda g: (0, 0)),
            pl.BlockSpec((ROWS, group), lambda g: (0, g)),
            pl.BlockSpec((ROWS, group), lambda g: (0, g)),
            pl.BlockSpec((ROWS, WIDTH), lambda g: (0, g)),
            pl.BlockSpec((ROWS, WIDTH), lambda g: (0, g)),
            pl.BlockSpec((per, 3, CHUNK, WIDTH), lambda g: (g, 0, 0, 0)),
        ],
        out_specs=(
            pl.BlockSpec((ROWS, group), lambda g: (0, g)),
            pl.BlockSpec((ROWS, group), lambda g: (0, g)),
            pl.BlockSpec((per, 4, CHUNK, WIDTH), lambda g: (g, 0, 0, 0)),
        ),
        scratch_shapes=[
            pltpu.VMEM((4 * ROWS, 2 * ROWS), jnp.float32),
            pltpu.VMEM((ROWS, ROWS), jnp.bfloat16),
        ],
        name="attend",
    )(block_path, assistant.reshape(1, ROWS), queries, grad_out, keys, values, far)

    small = jax.ShapeDtypeStruct(keys.shape, jnp.bfloat16)
    grad_keys, grad_values = pl.pallas_call(
        gather_kernel,
        out_shape=(small, small),
        in_specs=[smem(), vmem()],
        out_specs=(vmem(), vmem()),
        scratch_shapes=[two, two, wide, one, one, one, wide, one, one] + [sems] * 7,
        compiler_params=pltpu.CompilerParams(collective_id=1, has_side_effects=True),
        name="gather",
    )(block_path, grads)
    return attention, grad_queries, grad_keys, grad_values


def solution(mesh):
    rows = P(("leaf", "ctx"), None)
    in_specs = (rows, rows, rows, rows, P("leaf", None), P(("leaf", "ctx")))
    return jax.shard_map(
        on_device, mesh=mesh, in_specs=in_specs, out_specs=(rows,) * 4, check_vma=False
    )
```

```python
import functools
import math

import jax
import jax.numpy as jnp
from jax import lax
from jax.experimental import pallas as pl
from jax.experimental.pallas import tpu as pltpu
from jax.sharding import PartitionSpec as P

KEY_HEADS = 4
WIDTH = 128
GROUP = 8
ROWS = 128
NZ = 16
HALF = NZ // 2
PARTS = 4
CHUNK = ROWS // PARTS
CHUNKS = KEY_HEADS * 2 * PARTS
SCALE = 1.0 / math.sqrt(WIDTH)
EXP2_SCALE = SCALE * math.log2(math.e)
MASKED = -1e30


def place():
    me = lax.axis_index("ctx")
    return me, me // 2, lax.rem(me, 2)


def depth_of(paths, block):
    total = jnp.int32(-1)
    for e in range(4):
        total = total + (paths[block, e] >= 0).astype(jnp.int32)
    return total


def send(src, dst, send_sem, recv_sem, ctx):
    return pltpu.make_async_remote_copy(
        src_ref=src,
        dst_ref=dst,
        send_sem=send_sem,
        recv_sem=recv_sem,
        device_id={"ctx": ctx},
        device_id_type=pl.DeviceIdType.MESH,
    )


def greet(peers):
    barrier = pltpu.get_barrier_semaphore()
    for peer in peers:
        pl.semaphore_signal(
            barrier, inc=1, device_id={"ctx": peer}, device_id_type=pl.DeviceIdType.MESH
        )
    pl.semaphore_wait(barrier, len(peers))


def spread_kernel(
    paths, keys, values, slots, own, mate, root, seen, out,
    mate_send, mate_recv, root_send, root_recv, root_send2, chain_send, chain_recv,
):
    me, z, y = place()
    up = lax.rem(z + 1, NZ) * 2 + y
    down = lax.rem(z + NZ - 1, NZ) * 2 + y
    partner = z * 2 + 1 - y
    for h in range(KEY_HEADS):
        for t, ref in enumerate((keys, values)):
            first = (h * 2 + t) * PARTS
            own[first : first + PARTS] = ref[:, h * WIDTH : (h + 1) * WIDTH].reshape(
                PARTS, CHUNK, WIDTH
            )
    greet((up, down, partner))

    def to_mate(i):
        return send(own.at[i], mate.at[i], mate_send.at[i], mate_recv.at[i], partner)

    def to_next(i):
        return send(out.at[i], seen.at[i], chain_send.at[i], chain_recv.at[i], up)

    onward = jnp.where(z < HALF, up, down)

    def root_on(i):
        return send(root.at[i], root.at[i], root_send.at[i], root_recv.at[i], onward)

    def root_back(i):
        return send(root.at[i], root.at[i], root_send2.at[i], root_recv.at[i], down)

    @pl.loop(0, CHUNKS)
    def _(i):
        to_mate(i).start()

    d_own = depth_of(paths, me)
    d_mate = depth_of(paths, partner)

    def chain():
        @pl.loop(0, CHUNKS)
        def _(i):
            to_mate(i).wait_recv()
            mine = own[i]
            theirs = mate[i]

            @pl.when(z == 0)
            def _():
                seen[i, 0] = mine
                seen[i, 1] = mine

            @pl.when(z > 0)
            def _():
                to_next(i).wait_recv()

            for e in (1, 2):
                before = seen[i, e - 1]
                mate_hit = d_mate == e
                own_hit = d_own == e
                take_mate = mate_hit & ((y == 0) | (d_own != e))
                out[i, e - 1] = lax.select(
                    take_mate, theirs, lax.select(own_hit, mine, before)
                )
                slots[i, e] = lax.select(mate_hit & (y == 1), theirs, before)

            @pl.when(z < NZ - 1)
            def _():
                to_next(i).start()

    def roots():
        @pl.loop(0, CHUNKS)
        def _(i):
            @pl.when(z == 0)
            def _():
                root[i] = lax.select(y == 0, own[i], mate[i])

            @pl.when(z > 0)
            def _():
                root_on(i).wait_recv()

            slots[i, 0] = root[i]

            @pl.when((z != HALF - 1) & (z != HALF))
            def _():
                root_on(i).start()

            @pl.when(z == 0)
            def _():
                root_back(i).start()

    @pl.when(z >= HALF)
    def _():
        roots()

    chain()

    @pl.when(z < HALF)
    def _():
        roots()

    @pl.loop(0, CHUNKS)
    def _(i):
        to_mate(i).wait_send()

        @pl.when(z < NZ - 1)
        def _():
            to_next(i).wait_send()

        @pl.when((z != HALF - 1) & (z != HALF))
        def _():
            root_on(i).wait_send()

        @pl.when(z == 0)
        def _():
            root_back(i).wait_send()


def attend_kernel(
    paths, assistant, queries, grad_out, keys, values, far, attention, grad_queries, grads,
    bias, live,
):
    me, _, _ = place()
    cols = 2 * ROWS

    @pl.when(pl.program_id(0) == 0)
    def _():
        depth = depth_of(paths, me)
        for e in range(3):
            bias[e * ROWS : (e + 1) * ROWS] = jnp.full(
                (ROWS, cols), jnp.where(e < depth, 0.0, MASKED), jnp.float32
            )
        key_at = lax.broadcasted_iota(jnp.int32, (ROWS, cols), 0)
        row_at = lax.broadcasted_iota(jnp.int32, (ROWS, cols), 1)
        row_at = jnp.where(row_at >= ROWS, row_at - ROWS, row_at)
        bias[3 * ROWS :] = jnp.where(key_at <= row_at, 0.0, MASKED)
        r = lax.broadcasted_iota(jnp.int32, (ROWS, ROWS), 0)
        c = lax.broadcasted_iota(jnp.int32, (ROWS, ROWS), 1)
        spread = jnp.where(r == c, assistant[...].astype(jnp.float32), 0.0)
        live[...] = jnp.broadcast_to(
            jnp.sum(spread, axis=1, keepdims=True), (ROWS, ROWS)
        ).astype(jnp.bfloat16)

    far_keys = [far[0:PARTS, e].reshape(ROWS, WIDTH) for e in range(3)]
    far_values = [far[PARTS : 2 * PARTS, e].reshape(ROWS, WIDTH) for e in range(3)]
    k4 = jnp.concatenate(far_keys + [keys[...]], 0)
    v4 = jnp.concatenate(far_values + [values[...]], 0)
    k4t = k4.T
    v4t = v4.T
    dims = (((1,), (1,)), ((), ()))
    for pair in range(GROUP // 2):
        at = [slice((2 * pair + j) * WIDTH, (2 * pair + j + 1) * WIDTH) for j in range(2)]
        q2 = jnp.concatenate([queries[:, s] for s in at], 0)
        g2 = jnp.concatenate([grad_out[:, s] * live[...] for s in at], 0)
        s = lax.dot_general(k4, q2, dims, preferred_element_type=jnp.float32) + bias[...]
        top = jnp.max(s, axis=0, keepdims=True)
        p = jnp.exp2((s - top) * EXP2_SCALE)
        w = p * (1.0 / jnp.sum(p, axis=0, keepdims=True))
        wb = w.astype(jnp.bfloat16)
        out_t = jnp.dot(v4t, wb, preferred_element_type=jnp.float32)
        dp = lax.dot_general(v4, g2, dims, preferred_element_type=jnp.float32)
        out_t = out_t.astype(jnp.bfloat16)
        delta = jnp.sum(
            g2.T.astype(jnp.float32) * out_t.astype(jnp.float32), axis=0, keepdims=True
        )
        ds = (w * (dp - delta)).astype(jnp.bfloat16)
        gq_t = jnp.dot(k4t, ds, preferred_element_type=jnp.float32) * SCALE
        out = out_t.T
        gq = gq_t.astype(jnp.bfloat16).T
        for j in range(2):
            attention[:, at[j]] = out[j * ROWS : (j + 1) * ROWS]
            grad_queries[:, at[j]] = gq[j * ROWS : (j + 1) * ROWS]
        dk = jnp.dot(ds, q2, preferred_element_type=jnp.float32)
        dv = jnp.dot(wb, g2, preferred_element_type=jnp.float32)
        for t, d in enumerate((dk * SCALE, dv)):
            for e in range(4):
                new = d[e * ROWS : (e + 1) * ROWS].reshape(PARTS, CHUNK, WIDTH)
                here = slice(t * PARTS, (t + 1) * PARTS)
                if pair == 0:
                    grads[here, e] = new
                else:
                    grads[here, e] += new


def gather_kernel(
    paths, grads, grad_keys, grad_values,
    seen, out, total, root_in, root_last, root_out, rooted, to_x, from_x,
    chain_send, chain_recv, root_send, root_recv, last_recv, x_send, x_recv,
):
    me, z, y = place()
    up = lax.rem(z + 1, NZ) * 2 + y
    down = lax.rem(z + NZ - 1, NZ) * 2 + y
    partner = z * 2 + 1 - y
    greet((up, down, partner))
    d0 = depth_of(paths, z * 2)
    d1 = depth_of(paths, z * 2 + 1)
    late = (y == 1).astype(jnp.float32)
    early = 1.0 - late
    hit0 = [(d0 == e).astype(jnp.float32) for e in (1, 2)]
    hit1 = [(d1 == e).astype(jnp.float32) for e in (1, 2)]

    def to_next(i):
        return send(out.at[i], seen.at[i], chain_send.at[i], chain_recv.at[i], down)

    def to_mate(i):
        return send(to_x.at[i], from_x.at[i], x_send.at[i], x_recv.at[i], partner)

    onward = jnp.where(z < HALF, down, up)

    def root_on(i):
        return send(root_out.at[i], root_in.at[i], root_send.at[i], root_recv.at[i], onward)

    def root_end(i):
        return send(root_out.at[i], root_last.at[i], root_send.at[i], last_recv.at[i], onward)

    def chain():
        @pl.loop(0, CHUNKS)
        def _(i):
            @pl.when(z == NZ - 1)
            def _():
                seen[i] = jnp.zeros((2, CHUNK, WIDTH), jnp.bfloat16)

            @pl.when(z < NZ - 1)
            def _():
                to_next(i).wait_recv()

            taken0 = rooted[i]
            taken1 = jnp.zeros((CHUNK, WIDTH), jnp.float32)
            for e in (1, 2):
                before = seen[i, e - 1].astype(jnp.float32)
                mine = grads[i, e]
                taken1 = taken1 + hit1[e - 1] * before
                mid = (1.0 - hit1[e - 1]) * before + late * mine
                taken0 = taken0 + hit0[e - 1] * mid
                out[i, e - 1] = ((1.0 - hit0[e - 1]) * mid + early * mine).astype(jnp.bfloat16)

            @pl.when(z > 0)
            def _():
                to_next(i).start()

            to_x[i] = (early * taken1 + late * taken0).astype(jnp.bfloat16)
            to_mate(i).start()
            total[i] = grads[i, 3] + (early * taken0 + late * taken1)

    def roots():
        @pl.loop(0, CHUNKS)
        def _(i):
            rooted[i] = jnp.zeros((CHUNK, WIDTH), jnp.float32)

            @pl.when((z == HALF - 1) | (z == HALF))
            def _():
                root_out[i] = grads[i, 0].astype(jnp.bfloat16)

            @pl.when((z != HALF - 1) & (z != HALF))
            def _():
                root_on(i).wait_recv()
                root_out[i] = (grads[i, 0] + root_in[i].astype(jnp.float32)).astype(jnp.bfloat16)

            @pl.when(z == 0)
            def _():
                root_end(i).wait_recv()
                rooted[i] = (
                    grads[i, 0]
                    + root_in[i].astype(jnp.float32)
                    + root_last[i].astype(jnp.float32)
                )

            @pl.when((z > 0) & (z < NZ - 1))
            def _():
                root_on(i).start()

            @pl.when(z == NZ - 1)
            def _():
                root_end(i).start()

    @pl.when(z < NZ - 1)
    def _():
        roots()

    @pl.when(z == NZ - 1)
    def _():
        rooted[...] = jnp.zeros_like(rooted)

    chain()

    @pl.when(z == NZ - 1)
    def _():
        roots()

    @pl.loop(0, CHUNKS)
    def _(i):
        to_mate(i).wait_recv()
        total[i] += from_x[i].astype(jnp.float32)

    for h in range(KEY_HEADS):
        for t, ref in enumerate((grad_keys, grad_values)):
            first = (h * 2 + t) * PARTS
            ref[:, h * WIDTH : (h + 1) * WIDTH] = (
                total[first : first + PARTS].reshape(ROWS, WIDTH).astype(jnp.bfloat16)
            )

    @pl.loop(0, CHUNKS)
    def _(i):
        to_mate(i).wait_send()

        @pl.when(z > 0)
        def _():
            to_next(i).wait_send()
            root_on(i).wait_send()


def vmem():
    return pl.BlockSpec(memory_space=pltpu.VMEM)


def smem():
    return pl.BlockSpec(memory_space=pltpu.SMEM)


def on_device(queries, keys, values, grad_out, block_path, assistant):
    sems = pltpu.SemaphoreType.DMA((CHUNKS,))
    one = pltpu.VMEM((CHUNKS, CHUNK, WIDTH), jnp.bfloat16)
    two = pltpu.VMEM((CHUNKS, 2, CHUNK, WIDTH), jnp.bfloat16)
    wide = pltpu.VMEM((CHUNKS, CHUNK, WIDTH), jnp.float32)
    far = pl.pallas_call(
        spread_kernel,
        out_shape=jax.ShapeDtypeStruct((CHUNKS, 3, CHUNK, WIDTH), jnp.bfloat16),
        in_specs=[smem(), vmem(), vmem()],
        out_specs=vmem(),
        scratch_shapes=[one, one, one, two, two] + [sems] * 7,
        compiler_params=pltpu.CompilerParams(collective_id=0, has_side_effects=True),
        name="spread",
    )(block_path, keys, values)

    group = GROUP * WIDTH
    per = 2 * PARTS
    attention, grad_queries, grads = pl.pallas_call(
        attend_kernel,
        grid=(KEY_HEADS,),
        out_shape=(
            jax.ShapeDtypeStruct(queries.shape, jnp.bfloat16),
            jax.ShapeDtypeStruct(queries.shape, jnp.bfloat16),
            jax.ShapeDtypeStruct((CHUNKS, 4, CHUNK, WIDTH), jnp.float32),
        ),
        in_specs=[
            smem(),
            pl.BlockSpec((1, ROWS), lambda g: (0, 0)),
            pl.BlockSpec((ROWS, group), lambda g: (0, g)),
            pl.BlockSpec((ROWS, group), lambda g: (0, g)),
            pl.BlockSpec((ROWS, WIDTH), lambda g: (0, g)),
            pl.BlockSpec((ROWS, WIDTH), lambda g: (0, g)),
            pl.BlockSpec((per, 3, CHUNK, WIDTH), lambda g: (g, 0, 0, 0)),
        ],
        out_specs=(
            pl.BlockSpec((ROWS, group), lambda g: (0, g)),
            pl.BlockSpec((ROWS, group), lambda g: (0, g)),
            pl.BlockSpec((per, 4, CHUNK, WIDTH), lambda g: (g, 0, 0, 0)),
        ),
        scratch_shapes=[
            pltpu.VMEM((4 * ROWS, 2 * ROWS), jnp.float32),
            pltpu.VMEM((ROWS, ROWS), jnp.bfloat16),
        ],
        name="attend",
    )(block_path, assistant.reshape(1, ROWS), queries, grad_out, keys, values, far)

    small = jax.ShapeDtypeStruct(keys.shape, jnp.bfloat16)
    grad_keys, grad_values = pl.pallas_call(
        gather_kernel,
        out_shape=(small, small),
        in_specs=[smem(), vmem()],
        out_specs=(vmem(), vmem()),
        scratch_shapes=[two, two, wide, one, one, one, wide, one, one] + [sems] * 7,
        compiler_params=pltpu.CompilerParams(collective_id=1, has_side_effects=True),
        name="gather",
    )(block_path, grads)
    return attention, grad_queries, grad_keys, grad_values


def solution(mesh):
    rows = P(("leaf", "ctx"), None)
    in_specs = (rows, rows, rows, rows, P("leaf", None), P(("leaf", "ctx")))
    return jax.shard_map(
        on_device, mesh=mesh, in_specs=in_specs, out_specs=(rows,) * 4, check_vma=False
    )
```

```python
import functools
import math

import jax
import jax.numpy as jnp
from jax import lax
from jax.experimental import pallas as pl
from jax.experimental.pallas import tpu as pltpu
from jax.sharding import PartitionSpec as P

KEY_HEADS = 4
WIDTH = 128
GROUP = 8
ROWS = 128
NZ = 16
HALF = NZ // 2
PARTS = 4
CHUNK = ROWS // PARTS
CHUNKS = KEY_HEADS * 2 * PARTS
SCALE = 1.0 / math.sqrt(WIDTH)
EXP2_SCALE = SCALE * math.log2(math.e)
MASKED = -1e30


def place():
    me = lax.axis_index("ctx")
    return me, me // 2, lax.rem(me, 2)


def chip():
    leaf = lax.axis_index("leaf")
    return leaf, lax.rem(leaf, 2) == 1


def depth_of(paths, block):
    total = jnp.int32(-1)
    for e in range(4):
        total = total + (paths[block, e] >= 0).astype(jnp.int32)
    return total


def depth_in(paths, block):
    at = lax.broadcasted_iota(jnp.int32, paths.shape, 0) == block
    return jnp.sum((at & (paths >= 0)).astype(jnp.int32)) - 1


def send(src, dst, send_sem, recv_sem, ctx, leaf=None):
    device = {"ctx": ctx} if leaf is None else {"leaf": leaf, "ctx": ctx}
    return pltpu.make_async_remote_copy(
        src_ref=src,
        dst_ref=dst,
        send_sem=send_sem,
        recv_sem=recv_sem,
        device_id=device,
        device_id_type=pl.DeviceIdType.MESH,
    )


def greet(peers):
    barrier = pltpu.get_barrier_semaphore()
    for peer, leaf in peers:
        pl.semaphore_signal(
            barrier,
            inc=1,
            device_id={"leaf": leaf, "ctx": peer},
            device_id_type=pl.DeviceIdType.MESH,
        )
    pl.semaphore_wait(barrier, len(peers))


def meet(leaf, relay, buddy, me, up, down, partner):
    @pl.when(relay)
    def _():
        greet(((up, leaf), (down, leaf), (partner, leaf), (me, buddy), (partner, buddy)))

    @pl.when(jnp.logical_not(relay))
    def _():
        greet(((me, buddy), (partner, buddy)))


def spread_kernel(
    paths, keys, values, slots, pathv, own, mate, root, seen, out, ready,
    path_send, path_recv, own_send, own_recv, mate_send, mate_recv,
    root_send, root_recv, root_send2, chain_send, chain_recv, ready_send, ready_recv,
):
    me, z, y = place()
    leaf, relay = chip()
    buddy = jnp.where(relay, leaf - 1, leaf + 1)
    up = lax.rem(z + 1, NZ) * 2 + y
    down = lax.rem(z + NZ - 1, NZ) * 2 + y
    partner = z * 2 + 1 - y

    def fill(t):
        for h in range(KEY_HEADS):
            for k, ref in enumerate((keys, values)):
                first = (h * 2 + k) * PARTS
                own[first : first + PARTS, t] = ref[:, h * WIDTH : (h + 1) * WIDTH].reshape(
                    PARTS, CHUNK, WIDTH
                )
        pathv[t] = paths[...]

    @pl.when(relay)
    def _():
        fill(1)

    @pl.when(jnp.logical_not(relay))
    def _():
        fill(0)

    meet(leaf, relay, buddy, me, up, down, partner)

    def path_over():
        return send(pathv.at[0], pathv.at[0], path_send, path_recv, me, buddy)

    def own_over(i):
        return send(own.at[i, 0], own.at[i, 0], own_send.at[i], own_recv.at[i], me, buddy)

    def mate_over(i):
        return send(
            own.at[i, 0], mate.at[i, 0], mate_send.at[0, i], mate_recv.at[0, i], partner, buddy
        )

    def to_mate(i):
        return send(own.at[i, 1], mate.at[i, 1], mate_send.at[1, i], mate_recv.at[1, i], partner)

    def hand(i):
        return send(ready.at[i], slots.at[i], ready_send.at[i], ready_recv.at[i], me, buddy)

    def to_next(i):
        return send(out.at[i], seen.at[i], chain_send.at[i], chain_recv.at[i], up)

    onward = jnp.where(z < HALF, up, down)

    def root_on(i):
        return send(root.at[i], root.at[i], root_send.at[i], root_recv.at[i], onward)

    def root_back(i):
        return send(root.at[i], root.at[i], root_send2.at[i], root_recv.at[i], down)

    @pl.when(jnp.logical_not(relay))
    def _():
        path_over().start()

        @pl.loop(0, CHUNKS)
        def _(i):
            own_over(i).start()
            mate_over(i).start()

        path_over().wait_send()

        @pl.loop(0, CHUNKS)
        def _(i):
            hand(i).wait_recv()
            own_over(i).wait_send()
            mate_over(i).wait_send()

    roots_first = z > HALF

    def chain():
        path_over().wait_recv()
        d_own = [depth_in(pathv[t], me) for t in range(2)]
        d_mate = [depth_in(pathv[t], partner) for t in range(2)]

        @pl.loop(0, CHUNKS)
        def _(i):
            own_over(i).wait_recv()
            mate_over(i).wait_recv()
            to_mate(i).wait_recv()

            @pl.when(z == 0)
            def _():
                for t in range(2):
                    for e in range(2):
                        seen[i, t, e] = own[i, t]

            @pl.when(z > 0)
            def _():
                to_next(i).wait_recv()

            for t in range(2):
                mine = own[i, t]
                theirs = mate[i, t]
                for e in (1, 2):
                    before = seen[i, t, e - 1]
                    take_mate = (d_mate[t] == e) & ((y == 0) | (d_own[t] != e))
                    out[i, t, e - 1] = lax.select(
                        take_mate, theirs, lax.select(d_own[t] == e, mine, before)
                    )

            @pl.when(z < NZ - 1)
            def _():
                to_next(i).start()

            for t, ref in enumerate((ready, slots)):
                for e in (1, 2):
                    ref[i, e] = lax.select(
                        (d_mate[t] == e) & (y == 1), mate[i, t], seen[i, t, e - 1]
                    )

            @pl.when(roots_first)
            def _():
                hand(i).start()

    def roots():
        @pl.loop(0, CHUNKS)
        def _(i):
            @pl.when(z == 0)
            def _():
                for t in range(2):
                    root[i, t] = lax.select(y == 0, own[i, t], mate[i, t])

            @pl.when(z > 0)
            def _():
                root_on(i).wait_recv()

            @pl.when((z != HALF - 1) & (z != HALF))
            def _():
                root_on(i).start()

            @pl.when(z == 0)
            def _():
                root_back(i).start()

            ready[i, 0] = root[i, 0]
            slots[i, 0] = root[i, 1]

            @pl.when(jnp.logical_not(roots_first))
            def _():
                hand(i).start()

    @pl.when(relay)
    def _():
        @pl.loop(0, CHUNKS)
        def _(i):
            to_mate(i).start()

        @pl.when(roots_first)
        def _():
            roots()

        chain()

        @pl.when(jnp.logical_not(roots_first))
        def _():
            roots()

        @pl.loop(0, CHUNKS)
        def _(i):
            to_mate(i).wait_send()
            hand(i).wait_send()

            @pl.when(z < NZ - 1)
            def _():
                to_next(i).wait_send()

            @pl.when((z != HALF - 1) & (z != HALF))
            def _():
                root_on(i).wait_send()

            @pl.when(z == 0)
            def _():
                root_back(i).wait_send()


def attend_kernel(
    paths, assistant, queries, grad_out, keys, values, far, attention, grad_queries, grads,
    bias, live,
):
    me, _, _ = place()
    cols = 2 * ROWS

    @pl.when(pl.program_id(0) == 0)
    def _():
        depth = depth_of(paths, me)
        for e in range(3):
            bias[e * ROWS : (e + 1) * ROWS] = jnp.full(
                (ROWS, cols), jnp.where(e < depth, 0.0, MASKED), jnp.float32
            )
        key_at = lax.broadcasted_iota(jnp.int32, (ROWS, cols), 0)
        row_at = lax.broadcasted_iota(jnp.int32, (ROWS, cols), 1)
        row_at = jnp.where(row_at >= ROWS, row_at - ROWS, row_at)
        bias[3 * ROWS :] = jnp.where(key_at <= row_at, 0.0, MASKED)
        r = lax.broadcasted_iota(jnp.int32, (ROWS, ROWS), 0)
        c = lax.broadcasted_iota(jnp.int32, (ROWS, ROWS), 1)
        spread = jnp.where(r == c, assistant[...].astype(jnp.float32), 0.0)
        live[...] = jnp.broadcast_to(
            jnp.sum(spread, axis=1, keepdims=True), (ROWS, ROWS)
        ).astype(jnp.bfloat16)

    far_keys = [far[0:PARTS, e].reshape(ROWS, WIDTH) for e in range(3)]
    far_values = [far[PARTS : 2 * PARTS, e].reshape(ROWS, WIDTH) for e in range(3)]
    k4 = jnp.concatenate(far_keys + [keys[...]], 0)
    v4 = jnp.concatenate(far_values + [values[...]], 0)
    k4t = k4.T
    v4t = v4.T
    dims = (((1,), (1,)), ((), ()))
    for pair in range(GROUP // 2):
        at = [slice((2 * pair + j) * WIDTH, (2 * pair + j + 1) * WIDTH) for j in range(2)]
        q2 = jnp.concatenate([queries[:, s] for s in at], 0)
        g2 = jnp.concatenate([grad_out[:, s] * live[...] for s in at], 0)
        s = lax.dot_general(k4, q2, dims, preferred_element_type=jnp.float32) + bias[...]
        top = jnp.max(s, axis=0, keepdims=True)
        p = jnp.exp2((s - top) * EXP2_SCALE)
        w = p * (1.0 / jnp.sum(p, axis=0, keepdims=True))
        wb = w.astype(jnp.bfloat16)
        out_t = jnp.dot(v4t, wb, preferred_element_type=jnp.float32)
        dp = lax.dot_general(v4, g2, dims, preferred_element_type=jnp.float32)
        out_t = out_t.astype(jnp.bfloat16)
        delta = jnp.sum(
            g2.T.astype(jnp.float32) * out_t.astype(jnp.float32), axis=0, keepdims=True
        )
        ds = (w * (dp - delta)).astype(jnp.bfloat16)
        gq_t = jnp.dot(k4t, ds, preferred_element_type=jnp.float32) * SCALE
        out = out_t.T
        gq = gq_t.astype(jnp.bfloat16).T
        for j in range(2):
            attention[:, at[j]] = out[j * ROWS : (j + 1) * ROWS]
            grad_queries[:, at[j]] = gq[j * ROWS : (j + 1) * ROWS]
        dk = jnp.dot(ds, q2, preferred_element_type=jnp.float32)
        dv = jnp.dot(wb, g2, preferred_element_type=jnp.float32)
        for t, d in enumerate((dk * SCALE, dv)):
            for e in range(4):
                new = d[e * ROWS : (e + 1) * ROWS].reshape(PARTS, CHUNK, WIDTH)
                here = slice(t * PARTS, (t + 1) * PARTS)
                if pair == 0:
                    grads[here, e] = new
                else:
                    grads[here, e] += new


def gather_kernel(
    paths, grads, grad_keys, grad_values,
    pathv, given, seen, out, total, root_in, root_last, root_out, rooted, to_x, from_x, taken,
    path_send, path_recv, give_send, give_recv, take_send, take_recv,
    chain_send, chain_recv, root_send, root_recv, last_recv, x_send, x_recv,
):
    me, z, y = place()
    leaf, relay = chip()
    buddy = jnp.where(relay, leaf - 1, leaf + 1)
    up = lax.rem(z + 1, NZ) * 2 + y
    down = lax.rem(z + NZ - 1, NZ) * 2 + y
    partner = z * 2 + 1 - y

    @pl.when(relay)
    def _():
        pathv[1] = paths[...]

    @pl.when(jnp.logical_not(relay))
    def _():
        pathv[0] = paths[...]

    meet(leaf, relay, buddy, me, up, down, partner)

    def path_over():
        return send(pathv.at[0], pathv.at[0], path_send, path_recv, me, buddy)

    def give(i):
        return send(
            grads.at[i, pl.ds(0, 3)], given.at[i], give_send.at[i], give_recv.at[i], me, buddy
        )

    def take(i):
        return send(taken.at[i], taken.at[i], take_send.at[i], take_recv.at[i], me, buddy)

    def to_next(i):
        return send(out.at[i], seen.at[i], chain_send.at[i], chain_recv.at[i], down)

    def to_mate(i):
        return send(
            to_x.at[i, 1], from_x.at[i], x_send.at[1, i], x_recv.at[i], partner
        )

    def to_mate_buddy(i):
        return send(
            to_x.at[i, 0], from_x.at[i], x_send.at[0, i], x_recv.at[i], partner, buddy
        )

    onward = jnp.where(z < HALF, down, up)

    def root_on(i):
        return send(root_out.at[i], root_in.at[i], root_send.at[i], root_recv.at[i], onward)

    def root_end(i):
        return send(root_out.at[i], root_last.at[i], root_send.at[i], last_recv.at[i], onward)

    def chain():
        late = (y == 1).astype(jnp.float32)
        early = 1.0 - late
        d0 = [depth_in(pathv[t], z * 2) for t in range(2)]
        d1 = [depth_in(pathv[t], z * 2 + 1) for t in range(2)]
        hit0 = [[(d0[t] == e).astype(jnp.float32) for e in (1, 2)] for t in range(2)]
        hit1 = [[(d1[t] == e).astype(jnp.float32) for e in (1, 2)] for t in range(2)]

        @pl.loop(0, CHUNKS)
        def _(i):
            @pl.when(z == NZ - 1)
            def _():
                give(i).wait_recv()
                seen[i] = jnp.zeros((2, 2, CHUNK, WIDTH), jnp.bfloat16)

            @pl.when(z < NZ - 1)
            def _():
                to_next(i).wait_recv()

            for t, grad in enumerate((given, grads)):
                for e in (1, 2):
                    before = seen[i, t, e - 1].astype(jnp.float32)
                    mine = grad[i, e]
                    mid = (1.0 - hit1[t][e - 1]) * before + late * mine
                    out[i, t, e - 1] = (
                        (1.0 - hit0[t][e - 1]) * mid + early * mine
                    ).astype(jnp.bfloat16)

            @pl.when(z > 0)
            def _():
                to_next(i).start()

            for t, grad in enumerate((given, grads)):
                taken0 = rooted[i, t]
                taken1 = jnp.zeros((CHUNK, WIDTH), jnp.float32)
                for e in (1, 2):
                    before = seen[i, t, e - 1].astype(jnp.float32)
                    mid = (1.0 - hit1[t][e - 1]) * before + late * grad[i, e]
                    taken1 = taken1 + hit1[t][e - 1] * before
                    taken0 = taken0 + hit0[t][e - 1] * mid
                to_x[i, t] = (early * taken1 + late * taken0).astype(jnp.bfloat16)
                if t == 0:
                    to_mate_buddy(i).start()
                    taken[i] = early * taken0 + late * taken1
                    take(i).start()
                else:
                    to_mate(i).start()
                    total[i] = grads[i, 3] + (early * taken0 + late * taken1)

    def roots():
        @pl.loop(0, CHUNKS)
        def _(i):
            @pl.when(z < NZ - 1)
            def _():
                give(i).wait_recv()

            rooted[i] = jnp.zeros((2, CHUNK, WIDTH), jnp.float32)

            @pl.when((z == HALF - 1) | (z == HALF))
            def _():
                for t, grad in enumerate((given, grads)):
                    root_out[i, t] = grad[i, 0].astype(jnp.bfloat16)

            @pl.when((z != HALF - 1) & (z != HALF))
            def _():
                root_on(i).wait_recv()
                for t, grad in enumerate((given, grads)):
                    root_out[i, t] = (
                        grad[i, 0] + root_in[i, t].astype(jnp.float32)
                    ).astype(jnp.bfloat16)

            @pl.when(z == 0)
            def _():
                root_end(i).wait_recv()
                for t, grad in enumerate((given, grads)):
                    rooted[i, t] = (
                        grad[i, 0]
                        + root_in[i, t].astype(jnp.float32)
                        + root_last[i, t].astype(jnp.float32)
                    )

            @pl.when((z > 0) & (z < NZ - 1))
            def _():
                root_on(i).start()

            @pl.when(z == NZ - 1)
            def _():
                root_end(i).start()

    @pl.when(relay)
    def _():
        path_over().wait_recv()

        @pl.when(z < NZ - 1)
        def _():
            roots()

        @pl.when(z == NZ - 1)
        def _():
            rooted[...] = jnp.zeros_like(rooted)

        chain()

        @pl.when(z == NZ - 1)
        def _():
            roots()

        @pl.loop(0, CHUNKS)
        def _(i):
            to_mate(i).wait_recv()
            total[i] += from_x[i].astype(jnp.float32)

    @pl.when(jnp.logical_not(relay))
    def _():
        path_over().start()

        @pl.loop(0, CHUNKS)
        def _(i):
            give(i).start()

        path_over().wait_send()

        @pl.loop(0, CHUNKS)
        def _(i):
            take(i).wait_recv()
            to_mate_buddy(i).wait_recv()
            total[i] = grads[i, 3] + (taken[i] + from_x[i].astype(jnp.float32))
            give(i).wait_send()

    for h in range(KEY_HEADS):
        for k, ref in enumerate((grad_keys, grad_values)):
            first = (h * 2 + k) * PARTS
            ref[:, h * WIDTH : (h + 1) * WIDTH] = (
                total[first : first + PARTS].reshape(ROWS, WIDTH).astype(jnp.bfloat16)
            )

    @pl.when(relay)
    def _():
        @pl.loop(0, CHUNKS)
        def _(i):
            to_mate(i).wait_send()
            to_mate_buddy(i).wait_send()
            take(i).wait_send()

            @pl.when(z > 0)
            def _():
                to_next(i).wait_send()
                root_on(i).wait_send()


def vmem():
    return pl.BlockSpec(memory_space=pltpu.VMEM)


def smem():
    return pl.BlockSpec(memory_space=pltpu.SMEM)


def on_device(queries, keys, values, grad_out, block_path, assistant):
    sem = pltpu.SemaphoreType.DMA
    sems = sem((CHUNKS,))
    both = sem((2, CHUNKS))

    def room(*lead, dtype=jnp.bfloat16):
        return pltpu.VMEM((CHUNKS, *lead, CHUNK, WIDTH), dtype)

    full = jnp.float32
    pathv = pltpu.VMEM((2, *block_path.shape), jnp.int32)
    far = pl.pallas_call(
        spread_kernel,
        out_shape=jax.ShapeDtypeStruct((CHUNKS, 3, CHUNK, WIDTH), jnp.bfloat16),
        in_specs=[vmem()] * 3,
        out_specs=vmem(),
        scratch_shapes=[pathv, room(2), room(2), room(2), room(2, 2), room(2, 2), room(3)]
        + [sem, sem, sems, sems, both, both]
        + [sems] * 7,
        compiler_params=pltpu.CompilerParams(collective_id=0, has_side_effects=True),
        name="spread",
    )(block_path, keys, values)

    group = GROUP * WIDTH
    per = 2 * PARTS
    attention, grad_queries, grads = pl.pallas_call(
        attend_kernel,
        grid=(KEY_HEADS,),
        out_shape=(
            jax.ShapeDtypeStruct(queries.shape, jnp.bfloat16),
            jax.ShapeDtypeStruct(queries.shape, jnp.bfloat16),
            jax.ShapeDtypeStruct((CHUNKS, 4, CHUNK, WIDTH), jnp.float32),
        ),
        in_specs=[
            smem(),
            pl.BlockSpec((1, ROWS), lambda g: (0, 0)),
            pl.BlockSpec((ROWS, group), lambda g: (0, g)),
            pl.BlockSpec((ROWS, group), lambda g: (0, g)),
            pl.BlockSpec((ROWS, WIDTH), lambda g: (0, g)),
            pl.BlockSpec((ROWS, WIDTH), lambda g: (0, g)),
            pl.BlockSpec((per, 3, CHUNK, WIDTH), lambda g: (g, 0, 0, 0)),
        ],
        out_specs=(
            pl.BlockSpec((ROWS, group), lambda g: (0, g)),
            pl.BlockSpec((ROWS, group), lambda g: (0, g)),
            pl.BlockSpec((per, 4, CHUNK, WIDTH), lambda g: (g, 0, 0, 0)),
        ),
        scratch_shapes=[
            pltpu.VMEM((4 * ROWS, 2 * ROWS), jnp.float32),
            pltpu.VMEM((ROWS, ROWS), jnp.bfloat16),
        ],
        name="attend",
    )(block_path, assistant.reshape(1, ROWS), queries, grad_out, keys, values, far)

    small = jax.ShapeDtypeStruct(keys.shape, jnp.bfloat16)
    grad_keys, grad_values = pl.pallas_call(
        gather_kernel,
        out_shape=(small, small),
        in_specs=[vmem()] * 2,
        out_specs=(vmem(), vmem()),
        scratch_shapes=[
            pathv, room(3, dtype=full), room(2, 2), room(2, 2), room(dtype=full),
            room(2), room(2), room(2), room(2, dtype=full), room(2), room(), room(dtype=full),
        ]
        + [sem, sem]
        + [sems] * 9
        + [both, sems],
        compiler_params=pltpu.CompilerParams(collective_id=1, has_side_effects=True),
        name="gather",
    )(block_path, grads)
    return attention, grad_queries, grad_keys, grad_values


def solution(mesh):
    rows = P(("leaf", "ctx"), None)
    in_specs = (rows, rows, rows, rows, P("leaf", None), P(("leaf", "ctx")))
    return jax.shard_map(
        on_device, mesh=mesh, in_specs=in_specs, out_specs=(rows,) * 4, check_vma=False
    )
```

```python
import functools
import math
import types

import jax
import jax.numpy as jnp
from jax import lax
from jax.experimental import pallas as pl
from jax.experimental.pallas import tpu as pltpu
from jax.sharding import PartitionSpec as P

KEY_HEADS = 4
WIDTH = 128
GROUP = 8
ROWS = 128
NZ = 16
UPPER = 10
PARTS = 4
CHUNK = ROWS // PARTS
PER_HEAD = 2 * PARTS
CHUNKS = KEY_HEADS * PER_HEAD
SCALE = 1.0 / math.sqrt(WIDTH)
EXP2_SCALE = SCALE * math.log2(math.e)
MASKED = -1e30


def place():
    me = lax.axis_index("ctx")
    return me, me // 2, lax.rem(me, 2)


def depth_in(paths, block):
    at = lax.broadcasted_iota(jnp.int32, paths.shape, 0) == block
    return jnp.sum((at & (paths >= 0)).astype(jnp.int32)) - 1


def send(src, dst, send_sem, recv_sem, ctx, leaf=None):
    device = {"ctx": ctx} if leaf is None else {"leaf": leaf, "ctx": ctx}
    return pltpu.make_async_remote_copy(
        src_ref=src,
        dst_ref=dst,
        send_sem=send_sem,
        recv_sem=recv_sem,
        device_id=device,
        device_id_type=pl.DeviceIdType.MESH,
    )


def greet(peers):
    barrier = pltpu.get_barrier_semaphore()
    for peer, leaf in peers:
        pl.semaphore_signal(
            barrier,
            inc=1,
            device_id={"leaf": leaf, "ctx": peer},
            device_id_type=pl.DeviceIdType.MESH,
        )
    pl.semaphore_wait(barrier, len(peers))


def scratch(trees):
    def room(*lead, dtype=jnp.bfloat16):
        return pltpu.VMEM((CHUNKS, *lead, CHUNK, WIDTH), dtype)

    full = jnp.float32
    wide = pltpu.VMEM((KEY_HEADS, ROWS, GROUP * WIDTH), jnp.bfloat16)
    sem = pltpu.SemaphoreType.DMA
    one = sem((CHUNKS,))
    two = sem((2, CHUNKS))
    heads = sem((KEY_HEADS,))
    return dict(
        qv=wide, gv=wide, av=wide, zv=wide,
        bias=pltpu.VMEM((4 * ROWS, 2 * ROWS), full),
        live=pltpu.VMEM((ROWS, ROWS), jnp.bfloat16),
        pathv=pltpu.VMEM((2, *trees), jnp.int32),
        own=room(2), mate=room(2), pre=room(2, 2), root=room(2), seen=room(2, 2), out=room(2, 2),
        ready=room(3), slots=room(3),
        grads=room(4, dtype=full), given=room(3, dtype=full), net=room(2, 2), net_in=room(2, 2),
        back=room(2, 2), back_out=room(2, 2), total=room(dtype=full),
        root_in=room(2), root_one=room(2), root_last=room(2), root_out=room(2),
        rooted=room(2, dtype=full), to_x=room(2), from_x=room(), taken=room(dtype=full),
        q_sem=heads, g_sem=heads, a_sem=heads, z_sem=heads,
        path_send=sem, path_recv=sem,
        own_send=one, own_recv=one, mate_send=one, mate_recv=two,
        pre_send=two, pre_recv0=two, pre_recv1=two,
        root_send=one, root_send2=one, root_recv=one,
        chain_send1=one, chain_send2=one, chain_recv=one, hand_send=one, hand_recv=one,
        give_send=one, give_recv=one, take_send=one, take_recv=one,
        net_send=one, net_recv=one, back_send1=one, back_send2=one, back_recv=one,
        sum_send=one, sum_recv=one, sum_recv1=one, sum_recv2=one, x_send=two, x_recv=one,
    )


def attend(h, c, r):
    first = h * PER_HEAD

    def block(at, offset, *where):
        return at[(pl.ds(first + offset, PARTS), *where)].reshape(ROWS, WIDTH)

    k4 = jnp.concatenate([block(r.slots, 0, e) for e in range(3)] + [block(r.own, 0, c)], 0)
    v4 = jnp.concatenate([block(r.slots, PARTS, e) for e in range(3)] + [block(r.own, PARTS, c)], 0)
    k4t = k4.T
    v4t = v4.T
    dims = (((1,), (1,)), ((), ()))
    for pair in range(GROUP // 2):
        at = [slice((2 * pair + j) * WIDTH, (2 * pair + j + 1) * WIDTH) for j in range(2)]
        q2 = jnp.concatenate([r.qv[h, :, s] for s in at], 0)
        g2 = jnp.concatenate([r.gv[h, :, s] * r.live[...] for s in at], 0)
        s = lax.dot_general(k4, q2, dims, preferred_element_type=jnp.float32) + r.bias[...]
        top = jnp.max(s, axis=0, keepdims=True)
        p = jnp.exp2((s - top) * EXP2_SCALE)
        w = p * (1.0 / jnp.sum(p, axis=0, keepdims=True))
        wb = w.astype(jnp.bfloat16)
        out_t = jnp.dot(v4t, wb, preferred_element_type=jnp.float32)
        dp = lax.dot_general(v4, g2, dims, preferred_element_type=jnp.float32)
        out_t = out_t.astype(jnp.bfloat16)
        delta = jnp.sum(
            g2.T.astype(jnp.float32) * out_t.astype(jnp.float32), axis=0, keepdims=True
        )
        ds = (w * (dp - delta)).astype(jnp.bfloat16)
        gq_t = jnp.dot(k4t, ds, preferred_element_type=jnp.float32) * SCALE
        out = out_t.T
        gq = gq_t.astype(jnp.bfloat16).T
        for j in range(2):
            r.av[h, :, at[j]] = out[j * ROWS : (j + 1) * ROWS]
            r.zv[h, :, at[j]] = gq[j * ROWS : (j + 1) * ROWS]
        dk = jnp.dot(ds, q2, preferred_element_type=jnp.float32)
        dv = jnp.dot(wb, g2, preferred_element_type=jnp.float32)
        for t, d in enumerate((dk * SCALE, dv)):
            for e in range(4):
                new = d[e * ROWS : (e + 1) * ROWS].reshape(PARTS, CHUNK, WIDTH)
                here = pl.ds(first + t * PARTS, PARTS)
                if pair == 0:
                    r.grads[here, e] = new
                else:
                    r.grads[here, e] += new


def prepare(depth, assistant, r):
    cols = 2 * ROWS
    for e in range(3):
        r.bias[e * ROWS : (e + 1) * ROWS] = jnp.full(
            (ROWS, cols), jnp.where(e < depth, 0.0, MASKED), jnp.float32
        )
    key_at = lax.broadcasted_iota(jnp.int32, (ROWS, cols), 0)
    row_at = lax.broadcasted_iota(jnp.int32, (ROWS, cols), 1)
    row_at = jnp.where(row_at >= ROWS, row_at - ROWS, row_at)
    r.bias[3 * ROWS :] = jnp.where(key_at <= row_at, 0.0, MASKED)
    i = lax.broadcasted_iota(jnp.int32, (ROWS, ROWS), 0)
    j = lax.broadcasted_iota(jnp.int32, (ROWS, ROWS), 1)
    spread = jnp.where(i == j, assistant[...].astype(jnp.float32), 0.0)
    r.live[...] = jnp.broadcast_to(
        jnp.sum(spread, axis=1, keepdims=True), (ROWS, ROWS)
    ).astype(jnp.bfloat16)


def step_kernel(names, paths, assistant, keys, values, queries, grad_out, *refs):
    attention, grad_queries, grad_keys, grad_values = refs[:4]
    r = types.SimpleNamespace(**dict(zip(names, refs[4:])))
    me, z, y = place()
    leaf = lax.axis_index("leaf")
    c = lax.rem(leaf, 2)
    relay = c == 1
    ends = jnp.logical_not(relay)
    buddy = jnp.where(relay, leaf - 1, leaf + 1)
    odd = lax.rem(z, 2) == 1
    even = jnp.logical_not(odd)
    upper = z >= UPPER
    lower = jnp.logical_not(upper)

    def at(dz, side=None):
        return lax.rem(z + dz + NZ, NZ) * 2 + (y if side is None else side)

    other = 1 - y
    partner = at(0, other)
    pair_z = jnp.where(odd, z - 1, z + 1)

    def column(h):
        return pl.ds(pl.multiple_of(h * GROUP * WIDTH, GROUP * WIDTH), GROUP * WIDTH)

    def q_in(h):
        return pltpu.make_async_copy(queries.at[:, column(h)], r.qv.at[h], r.q_sem.at[h])

    def g_in(h):
        return pltpu.make_async_copy(grad_out.at[:, column(h)], r.gv.at[h], r.g_sem.at[h])

    def a_out(h):
        return pltpu.make_async_copy(r.av.at[h], attention.at[:, column(h)], r.a_sem.at[h])

    def z_out(h):
        return pltpu.make_async_copy(r.zv.at[h], grad_queries.at[:, column(h)], r.z_sem.at[h])

    for h in range(KEY_HEADS):
        q_in(h).start()
        g_in(h).start()
    for h in range(KEY_HEADS):
        for k, ref in enumerate((keys, values)):
            first = (h * 2 + k) * PARTS
            r.own[first : first + PARTS, c] = ref[:, h * WIDTH : (h + 1) * WIDTH].reshape(
                PARTS, CHUNK, WIDTH
            )
    r.pathv[1] = paths[...]

    @pl.when(ends)
    def _():
        r.pathv[0] = paths[...]


    @pl.when(relay)
    def _():
        greet(
            (
                (at(1), leaf), (at(-1), leaf), (at(2), leaf), (at(-2), leaf), (partner, leaf),
                (pair_z * 2 + other, leaf), (me, buddy), (partner, buddy),
                (pair_z * 2 + y, buddy), (pair_z * 2 + other, buddy),
            )
        )

    @pl.when(ends)
    def _():
        greet(
            (
                (me, buddy), (partner, buddy),
                (pair_z * 2 + y, buddy), (pair_z * 2 + other, buddy),
            )
        )

    def path_over():
        return send(r.pathv.at[0], r.pathv.at[0], r.path_send, r.path_recv, me, buddy)

    def own_over(i):
        return send(r.own.at[i, 0], r.own.at[i, 0], r.own_send.at[i], r.own_recv.at[i], me, buddy)

    def to_mate(i, t):
        return send(
            r.own.at[i, t], r.mate.at[i, t], r.mate_send.at[i], r.mate_recv.at[t, i],
            partner, buddy if t == 0 else leaf,
        )

    def to_leader(i, t, j):
        recv = r.pre_recv0 if t == 0 else r.pre_recv1
        return send(
            r.own.at[i, t], r.pre.at[i, t, j], r.pre_send.at[j, i], recv.at[j, i],
            at(1, y if j == 0 else other), buddy if t == 0 else leaf,
        )

    def hand(i):
        return send(r.ready.at[i], r.slots.at[i], r.hand_send.at[i], r.hand_recv.at[i], me, buddy)

    def chain_one(i):
        return send(r.out.at[i], r.seen.at[i], r.chain_send1.at[i], r.chain_recv.at[i], at(1))

    def chain_two(i):
        return send(r.out.at[i], r.seen.at[i], r.chain_send2.at[i], r.chain_recv.at[i], at(2))

    def root_on(i):
        return send(
            r.root.at[i], r.root.at[i], r.root_send.at[i], r.root_recv.at[i],
            jnp.where(lower, at(1), at(-1)),
        )

    def root_back(i):
        return send(r.root.at[i], r.root.at[i], r.root_send2.at[i], r.root_recv.at[i], at(-1))

    def give(i):
        return send(
            r.grads.at[i, pl.ds(0, 3)], r.given.at[i], r.give_send.at[i], r.give_recv.at[i],
            me, buddy,
        )

    def take(i):
        return send(r.taken.at[i], r.taken.at[i], r.take_send.at[i], r.take_recv.at[i], me, buddy)

    def net_over(i):
        return send(r.net.at[i], r.net_in.at[i], r.net_send.at[i], r.net_recv.at[i], at(-1))

    def back_one(i):
        return send(r.back_out.at[i], r.back.at[i], r.back_send1.at[i], r.back_recv.at[i], at(-1))

    def back_two(i):
        return send(r.back_out.at[i], r.back.at[i], r.back_send2.at[i], r.back_recv.at[i], at(-2))

    def sum_on(i):
        return send(
            r.root_out.at[i], r.root_in.at[i], r.sum_send.at[i], r.sum_recv.at[i],
            jnp.where(lower, at(-2), at(1)),
        )

    def sum_one(i):
        return send(r.root_out.at[i], r.root_one.at[i], r.sum_send.at[i], r.sum_recv1.at[i], at(-1))

    def sum_last(i):
        return send(r.root_out.at[i], r.root_last.at[i], r.sum_send.at[i], r.sum_recv2.at[i], at(1))

    def x_over(i, t):
        return send(
            r.to_x.at[i, t], r.from_x.at[i], r.x_send.at[t, i], r.x_recv.at[i],
            partner, buddy if t == 0 else leaf,
        )

    def share(t):
        @pl.loop(0, CHUNKS)
        def _(i):
            to_mate(i, t).start()

            @pl.when(even)
            def _():
                for j in range(2):
                    to_leader(i, t, j).start()

    def shared(t):
        @pl.loop(0, CHUNKS)
        def _(i):
            to_mate(i, t).wait_send()

            @pl.when(even)
            def _():
                for j in range(2):
                    to_leader(i, t, j).wait_send()

    def store_results():
        for h in range(KEY_HEADS):
            for k, ref in enumerate((grad_keys, grad_values)):
                first = (h * 2 + k) * PARTS
                ref[:, h * WIDTH : (h + 1) * WIDTH] = (
                    r.total[first : first + PARTS].reshape(ROWS, WIDTH).astype(jnp.bfloat16)
                )
        for h in range(KEY_HEADS):
            a_out(h).wait()
            z_out(h).wait()

    def compute(h):
        q_in(h).wait()
        g_in(h).wait()
        attend(h, c, r)
        a_out(h).start()
        z_out(h).start()

    @pl.when(ends)
    def _():
        path_over().start()

        @pl.loop(0, CHUNKS)
        def _(i):
            own_over(i).start()

        share(0)

    @pl.when(relay)
    def _():
        share(1)

    prepare(depth_in(paths[...], me), assistant, r)

    @pl.when(relay)
    def _():
        path_over().wait_recv()

    deep = [
        [depth_in(r.pathv[t], b) for b in (z * 2 - 2, z * 2 - 1, z * 2, z * 2 + 1, z * 2 + 2, z * 2 + 3)]
        for t in range(2)
    ]

    def ahead(h):
        @pl.loop(0, PER_HEAD)
        def _(n):
            i = h * PER_HEAD + n
            own_over(i).wait_recv()
            for t in range(2):
                to_mate(i, t).wait_recv()

            @pl.when(z < 2)
            def _():
                for t in range(2):
                    for e in range(2):
                        r.seen[i, t, e] = r.own[i, t]

            @pl.when(odd)
            def _():
                for t in range(2):
                    for j in range(2):
                        to_leader(i, t, j).wait_recv()

            @pl.when(z > 1)
            def _():
                chain_one(i).wait_recv()

            @pl.when(odd)
            def _():
                for t in range(2):
                    d_a, d_b, d_0, d_1 = deep[t][:4]
                    near, far = r.pre[i, t, 0], r.pre[i, t, 1]
                    first = lax.select(y == 0, near, far)
                    second = lax.select(y == 0, far, near)
                    block0 = lax.select(y == 0, r.own[i, t], r.mate[i, t])
                    block1 = lax.select(y == 0, r.mate[i, t], r.own[i, t])
                    for e in (1, 2):
                        mid = lax.select(
                            d_b == e, second, lax.select(d_a == e, first, r.seen[i, t, e - 1])
                        )
                        r.out[i, t, e - 1] = lax.select(
                            d_1 == e, block1, lax.select(d_0 == e, block0, mid)
                        )
                        r.seen[i, t, e - 1] = mid

            @pl.when(odd & (z < NZ - 1))
            def _():
                chain_one(i).start()

            @pl.when(odd & (z < NZ - 2))
            def _():
                chain_two(i).start()

            for t, ref in enumerate((r.ready, r.slots)):
                for e in (1, 2):
                    ref[i, e] = lax.select(
                        (deep[t][2] == e) & (y == 1), r.mate[i, t], r.seen[i, t, e - 1]
                    )

            @pl.when(upper)
            def _():
                hand(i).start()

    def roots():
        @pl.loop(0, CHUNKS)
        def _(i):
            @pl.when(z == 0)
            def _():
                for t in range(2):
                    r.root[i, t] = lax.select(y == 0, r.own[i, t], r.mate[i, t])

            @pl.when(z > 0)
            def _():
                root_on(i).wait_recv()

            @pl.when((z != UPPER - 1) & (z != UPPER))
            def _():
                root_on(i).start()

            @pl.when(z == 0)
            def _():
                root_back(i).start()

            r.ready[i, 0] = r.root[i, 0]
            r.slots[i, 0] = r.root[i, 1]

            @pl.when(lower)
            def _():
                hand(i).start()

    late = (y == 1).astype(jnp.float32)
    early = 1.0 - late

    def keep(t, n):
        return [(deep[t][n] != e).astype(jnp.float32) for e in (1, 2)]

    def nets(h):
        @pl.loop(0, PER_HEAD)
        def _(n):
            i = h * PER_HEAD + n
            give(i).wait_recv()

            @pl.when(odd)
            def _():
                for t, grad in enumerate((r.given, r.grads)):
                    for e in (1, 2):
                        factor = late * keep(t, 2)[e - 1] + early
                        r.net[i, t, e - 1] = (factor * grad[i, e]).astype(jnp.bfloat16)
                net_over(i).start()

    def sums(h):
        @pl.loop(0, PER_HEAD)
        def _(n):
            i = h * PER_HEAD + n
            r.rooted[i] = jnp.zeros((2, CHUNK, WIDTH), jnp.float32)
            starts = (z == UPPER) | (z == UPPER - 1) | (z == UPPER - 2)

            @pl.when(starts)
            def _():
                for t, grad in enumerate((r.given, r.grads)):
                    r.root_out[i, t] = grad[i, 0].astype(jnp.bfloat16)

            @pl.when(jnp.logical_not(starts))
            def _():
                sum_on(i).wait_recv()
                for t, grad in enumerate((r.given, r.grads)):
                    r.root_out[i, t] = (
                        grad[i, 0] + r.root_in[i, t].astype(jnp.float32)
                    ).astype(jnp.bfloat16)

            @pl.when(z == 0)
            def _():
                sum_one(i).wait_recv()
                sum_last(i).wait_recv()
                for t, grad in enumerate((r.given, r.grads)):
                    r.rooted[i, t] = (
                        (grad[i, 0] + r.root_in[i, t].astype(jnp.float32))
                        + (r.root_one[i, t].astype(jnp.float32)
                           + r.root_last[i, t].astype(jnp.float32))
                    )

            @pl.when((z > 1) & (z < NZ - 1))
            def _():
                sum_on(i).start()

            @pl.when(z == 1)
            def _():
                sum_one(i).start()

            @pl.when(z == NZ - 1)
            def _():
                sum_last(i).start()

    def backward(h):
        @pl.loop(0, PER_HEAD)
        def _(n):
            i = h * PER_HEAD + n

            @pl.when(z >= NZ - 2)
            def _():
                r.back[i] = jnp.zeros((2, 2, CHUNK, WIDTH), jnp.bfloat16)

            @pl.when(z < NZ - 2)
            def _():
                back_one(i).wait_recv()

            @pl.when(even)
            def _():
                net_over(i).wait_recv()
                for t, grad in enumerate((r.given, r.grads)):
                    k0, k1, k2, k3 = (keep(t, n) for n in (2, 3, 4, 5))
                    for e in (1, 2):
                        mid = (k2[e - 1] * k3[e - 1]) * r.back[i, t, e - 1].astype(
                            jnp.float32
                        ) + r.net_in[i, t, e - 1].astype(jnp.float32)
                        mine = grad[i, e]
                        after = k1[e - 1] * mid + late * mine
                        r.back_out[i, t, e - 1] = (
                            k0[e - 1] * after + early * mine
                        ).astype(jnp.bfloat16)

            @pl.when(even & (z > 0))
            def _():
                back_one(i).start()
                back_two(i).start()

            use_net = even.astype(jnp.float32)
            for t, grad in enumerate((r.given, r.grads)):
                k0, k1, k2, k3 = (keep(t, n) for n in (2, 3, 4, 5))
                taken0 = r.rooted[i, t]
                taken1 = jnp.zeros((CHUNK, WIDTH), jnp.float32)
                for e in (1, 2):
                    factor = use_net * (k2[e - 1] * k3[e - 1]) + (1.0 - use_net)
                    before = factor * r.back[i, t, e - 1].astype(jnp.float32)
                    before = before + use_net * r.net_in[i, t, e - 1].astype(jnp.float32)
                    taken1 = taken1 + (1.0 - k1[e - 1]) * before
                    after = k1[e - 1] * before + late * grad[i, e]
                    taken0 = taken0 + (1.0 - k0[e - 1]) * after
                r.to_x[i, t] = (early * taken1 + late * taken0).astype(jnp.bfloat16)
                x_over(i, t).start()
                mine = early * taken0 + late * taken1
                if t == 0:
                    r.taken[i] = mine
                    take(i).start()
                else:
                    r.total[i] = r.grads[i, 3] + mine

    @pl.when(odd)
    def _():
        r.net_in[...] = jnp.zeros_like(r.net_in)

    @pl.when(relay)
    def _():
        r.rooted[...] = jnp.zeros_like(r.rooted)

        @pl.when(lower)
        def _():
            @pl.loop(0, KEY_HEADS)
            def _(h):
                ahead(h)

        roots()

    @pl.when(ends)
    def _():
        path_over().wait_send()

    lag = jnp.where(z >= 12, jnp.minimum(NZ - z, 3), KEY_HEADS)

    @pl.loop(0, 2 * KEY_HEADS)
    def _(s):
        @pl.when(relay)
        def _():
            @pl.when(upper & (s < KEY_HEADS))
            def _():
                ahead(s)

            @pl.when((s >= 1) & (s <= KEY_HEADS))
            def _():
                nets(s - 1)

            @pl.when(lower & (s == KEY_HEADS))
            def _():
                @pl.loop(0, KEY_HEADS)
                def _(h):
                    sums(h)

            @pl.when((s >= lag) & (s < lag + KEY_HEADS))
            def _():
                backward(s - lag)

            @pl.when(upper & (s >= 1) & (s <= KEY_HEADS))
            def _():
                sums(s - 1)

        @pl.when(s < KEY_HEADS)
        def _():
            @pl.when(ends)
            def _():
                @pl.loop(0, PER_HEAD)
                def _(n):
                    hand(s * PER_HEAD + n).wait_recv()

            compute(s)

            @pl.when(ends)
            def _():
                @pl.loop(0, PER_HEAD)
                def _(n):
                    give(s * PER_HEAD + n).start()

    @pl.when(relay)
    def _():
        @pl.loop(0, CHUNKS)
        def _(i):
            x_over(i, 1).wait_recv()
            r.total[i] += r.from_x[i].astype(jnp.float32)

    @pl.when(ends)
    def _():
        @pl.loop(0, CHUNKS)
        def _(i):
            take(i).wait_recv()
            x_over(i, 0).wait_recv()
            r.total[i] = r.grads[i, 3] + (r.taken[i] + r.from_x[i].astype(jnp.float32))

    store_results()

    @pl.when(ends)
    def _():
        shared(0)

        @pl.loop(0, CHUNKS)
        def _(i):
            own_over(i).wait_send()
            give(i).wait_send()

    @pl.when(relay)
    def _():
        shared(1)

        @pl.loop(0, CHUNKS)
        def _(i):
            hand(i).wait_send()
            take(i).wait_send()
            for t in range(2):
                x_over(i, t).wait_send()

            @pl.when((z != UPPER - 1) & (z != UPPER))
            def _():
                root_on(i).wait_send()

            @pl.when(z == 0)
            def _():
                root_back(i).wait_send()

            @pl.when(z > 0)
            def _():
                sum_on(i).wait_send()

            @pl.when(odd & (z < NZ - 1))
            def _():
                chain_one(i).wait_send()

            @pl.when(odd & (z < NZ - 2))
            def _():
                chain_two(i).wait_send()

            @pl.when(odd)
            def _():
                net_over(i).wait_send()

            @pl.when(even & (z > 0))
            def _():
                back_one(i).wait_send()
                back_two(i).wait_send()


def on_device(queries, keys, values, grad_out, block_path, assistant):
    extra = scratch(block_path.shape)
    vmem = pl.BlockSpec(memory_space=pltpu.VMEM)
    anywhere = pl.BlockSpec(memory_space=pl.ANY)
    wide = jax.ShapeDtypeStruct(queries.shape, jnp.bfloat16)
    small = jax.ShapeDtypeStruct(keys.shape, jnp.bfloat16)
    return pl.pallas_call(
        functools.partial(step_kernel, tuple(extra)),
        out_shape=(wide, wide, small, small),
        in_specs=[vmem] * 4 + [anywhere] * 2,
        out_specs=(anywhere, anywhere, vmem, vmem),
        scratch_shapes=list(extra.values()),
        compiler_params=pltpu.CompilerParams(collective_id=0, has_side_effects=True),
        name="step",
    )(block_path, assistant.reshape(1, ROWS), keys, values, queries, grad_out)


def solution(mesh):
    rows = P(("leaf", "ctx"), None)
    in_specs = (rows, rows, rows, rows, P("leaf", None), P(("leaf", "ctx")))
    return jax.shard_map(
        on_device, mesh=mesh, in_specs=in_specs, out_specs=(rows,) * 4, check_vma=False
    )
```

```python
import functools
import math
import types

import jax
import jax.numpy as jnp
from jax import lax
from jax.experimental import pallas as pl
from jax.experimental.pallas import tpu as pltpu
from jax.sharding import PartitionSpec as P

KEY_HEADS = 4
WIDTH = 128
GROUP = 8
ROWS = 128
NZ = 16
UPPER = 10
ROOT_UP = 5
PARTS = 2
CHUNK = ROWS // PARTS
PER_HEAD = 2 * PARTS
CHUNKS = KEY_HEADS * PER_HEAD
SCALE = 1.0 / math.sqrt(WIDTH)
EXP2_SCALE = SCALE * math.log2(math.e)
MASKED = -1e30


def place():
    me = lax.axis_index("ctx")
    return me, me // 2, lax.rem(me, 2)


def depth_in(paths, block):
    at = lax.broadcasted_iota(jnp.int32, paths.shape, 1) == block
    return jnp.sum((at & (paths >= 0)).astype(jnp.int32)) - 1


def send(src, dst, send_sem, recv_sem, ctx, leaf=None):
    device = {"ctx": ctx} if leaf is None else {"leaf": leaf, "ctx": ctx}
    return pltpu.make_async_remote_copy(
        src_ref=src,
        dst_ref=dst,
        send_sem=send_sem,
        recv_sem=recv_sem,
        device_id=device,
        device_id_type=pl.DeviceIdType.MESH,
    )


def greet(peers):
    barrier = pltpu.get_barrier_semaphore()
    for peer, leaf in peers:
        pl.semaphore_signal(
            barrier,
            inc=1,
            device_id={"leaf": leaf, "ctx": peer},
            device_id_type=pl.DeviceIdType.MESH,
        )
    pl.semaphore_wait(barrier, len(peers))


def scratch(trees):
    def room(*lead, dtype=jnp.bfloat16):
        return pltpu.VMEM((CHUNKS, *lead, CHUNK, WIDTH), dtype)

    full = jnp.float32
    wide = pltpu.VMEM((KEY_HEADS, ROWS, GROUP * WIDTH), jnp.bfloat16)
    sem = pltpu.SemaphoreType.DMA
    one = sem((CHUNKS,))
    two = sem((2, CHUNKS))
    heads = sem((KEY_HEADS,))
    return dict(
        qv=wide, gv=wide, av=wide, zv=wide,
        bias=pltpu.VMEM((4 * ROWS, 2 * ROWS), full),
        live=pltpu.VMEM((ROWS, ROWS), jnp.bfloat16),
        pathv=pltpu.VMEM((2, *trees), jnp.int32),
        own=room(2), mate=room(2), pair=room(2), pre=room(2), root=room(2),
        seen=room(2), out=room(2), base=room(2), side=room(2),
        ready=room(2), slots=room(3),
        grads=room(4, dtype=full), given=room(3, dtype=full), swap=room(2), swap_in=room(2),
        net=room(2), net_in=room(2), back=room(2), back_out=room(2), total=room(dtype=full),
        root_in=room(2), root_last=room(2), root_out=room(2),
        rooted=room(2, dtype=full), ra=room(dtype=full), rb=room(dtype=full), zero=room(dtype=full), to_x=room(2), from_x=room(), taken=room(dtype=full),
        q_sem=heads, g_sem=heads, a_sem=heads, z_sem=heads,
        path_send=sem, path_recv=sem,
        own_send=one, own_recv=one, mate_send=one, mate_recv=two,
        pre_send=one, pre_recv=one, side_send=one, side_recv=one, swap_send=one, swap_recv=one,
        root_send=one, root_send1=one, root_send2=one, root_send3=one, over_send=one, over_recv=one,
        zero_send=one, zero_recv=one, ra_send=one, ra_recv=one, rb_send=two, rb_recv=one, root_recv=one,
        chain_send1=one, chain_send2=one, chain_recv=one, hand_send=one, hand_recv=one,
        give_send=one, give_recv=one, take_send=one, take_recv=one,
        net_send=one, net_recv=one, back_send1=one, back_send2=one, back_recv=one,
        sum_send=one, sum_recv=one, sum_recv2=one, x_send=two, x_recv=one,
    )


def attend(h, c, r):
    first = h * PER_HEAD

    def block(at, offset, *where):
        return at[(pl.ds(first + offset, PARTS), *where)].reshape(ROWS, WIDTH)

    k4 = jnp.concatenate([block(r.slots, 0, e) for e in range(3)] + [block(r.own, 0, c)], 0)
    v4 = jnp.concatenate([block(r.slots, PARTS, e) for e in range(3)] + [block(r.own, PARTS, c)], 0)
    k4t = k4.T
    v4t = v4.T
    dims = (((1,), (1,)), ((), ()))
    for pair in range(GROUP // 2):
        at = [slice((2 * pair + j) * WIDTH, (2 * pair + j + 1) * WIDTH) for j in range(2)]
        q2 = jnp.concatenate([r.qv[h, :, s] for s in at], 0)
        g2 = jnp.concatenate([r.gv[h, :, s] * r.live[...] for s in at], 0)
        s = lax.dot_general(k4, q2, dims, preferred_element_type=jnp.float32) + r.bias[...]
        top = jnp.max(s, axis=0, keepdims=True)
        p = jnp.exp2((s - top) * EXP2_SCALE)
        w = p * (1.0 / jnp.sum(p, axis=0, keepdims=True))
        wb = w.astype(jnp.bfloat16)
        out_t = jnp.dot(v4t, wb, preferred_element_type=jnp.float32)
        dp = lax.dot_general(v4, g2, dims, preferred_element_type=jnp.float32)
        out_t = out_t.astype(jnp.bfloat16)
        delta = jnp.sum(
            g2.T.astype(jnp.float32) * out_t.astype(jnp.float32), axis=0, keepdims=True
        )
        ds = (w * (dp - delta)).astype(jnp.bfloat16)
        gq_t = jnp.dot(k4t, ds, preferred_element_type=jnp.float32) * SCALE
        out = out_t.T
        gq = gq_t.astype(jnp.bfloat16).T
        for j in range(2):
            r.av[h, :, at[j]] = out[j * ROWS : (j + 1) * ROWS]
            r.zv[h, :, at[j]] = gq[j * ROWS : (j + 1) * ROWS]
        dk = jnp.dot(ds, q2, preferred_element_type=jnp.float32)
        dv = jnp.dot(wb, g2, preferred_element_type=jnp.float32)
        for t, d in enumerate((dk * SCALE, dv)):
            for e in range(4):
                new = d[e * ROWS : (e + 1) * ROWS].reshape(PARTS, CHUNK, WIDTH)
                here = pl.ds(first + t * PARTS, PARTS)
                if pair == 0:
                    r.grads[here, e] = new
                else:
                    r.grads[here, e] += new


def prepare(depth, assistant, r):
    cols = 2 * ROWS
    for e in range(3):
        r.bias[e * ROWS : (e + 1) * ROWS] = jnp.full(
            (ROWS, cols), jnp.where(e < depth, 0.0, MASKED), jnp.float32
        )
    key_at = lax.broadcasted_iota(jnp.int32, (ROWS, cols), 0)
    row_at = lax.broadcasted_iota(jnp.int32, (ROWS, cols), 1)
    row_at = jnp.where(row_at >= ROWS, row_at - ROWS, row_at)
    r.bias[3 * ROWS :] = jnp.where(key_at <= row_at, 0.0, MASKED)
    i = lax.broadcasted_iota(jnp.int32, (ROWS, ROWS), 0)
    j = lax.broadcasted_iota(jnp.int32, (ROWS, ROWS), 1)
    spread = jnp.where(i == j, assistant[...].astype(jnp.float32), 0.0)
    r.live[...] = jnp.broadcast_to(
        jnp.sum(spread, axis=1, keepdims=True), (ROWS, ROWS)
    ).astype(jnp.bfloat16)


def step_kernel(names, paths, assistant, keys, values, queries, grad_out, *refs):
    attention, grad_queries, grad_keys, grad_values = refs[:4]
    r = types.SimpleNamespace(**dict(zip(names, refs[4:])))
    me, z, y = place()
    leaf = lax.axis_index("leaf")
    c = lax.rem(leaf, 2)
    relay = c == 1
    ends = jnp.logical_not(relay)
    buddy = jnp.where(relay, leaf - 1, leaf + 1)
    odd = lax.rem(z, 2) == 1
    even = jnp.logical_not(odd)
    upper = z >= UPPER
    lower = jnp.logical_not(upper)

    def at(dz, side=None):
        return lax.rem(z + dz + NZ, NZ) * 2 + (y if side is None else side)

    other = 1 - y
    partner = at(0, other)
    lane = 1 + y
    far_lane = 2 - y

    def column(h):
        return pl.ds(pl.multiple_of(h * GROUP * WIDTH, GROUP * WIDTH), GROUP * WIDTH)

    def q_in(h):
        return pltpu.make_async_copy(queries.at[:, column(h)], r.qv.at[h], r.q_sem.at[h])

    def g_in(h):
        return pltpu.make_async_copy(grad_out.at[:, column(h)], r.gv.at[h], r.g_sem.at[h])

    def a_out(h):
        return pltpu.make_async_copy(r.av.at[h], attention.at[:, column(h)], r.a_sem.at[h])

    def z_out(h):
        return pltpu.make_async_copy(r.zv.at[h], grad_queries.at[:, column(h)], r.z_sem.at[h])

    for h in range(KEY_HEADS):
        q_in(h).start()
        g_in(h).start()
    for h in range(KEY_HEADS):
        for k, ref in enumerate((keys, values)):
            first = (h * 2 + k) * PARTS
            r.own[first : first + PARTS, c] = ref[:, h * WIDTH : (h + 1) * WIDTH].reshape(
                PARTS, CHUNK, WIDTH
            )
    r.pathv[1] = paths[...]

    @pl.when(ends)
    def _():
        r.pathv[0] = paths[...]


    greet(
        (
            (at(1), leaf), (at(-1), leaf), (at(2), leaf), (at(-2), leaf), (partner, leaf),
            (me, buddy), (partner, buddy), (at(1), buddy), (at(-1), buddy),
            (at(2), buddy), (at(-2), buddy),
        )
    )

    def path_over():
        return send(r.pathv.at[0], r.pathv.at[0], r.path_send, r.path_recv, me, buddy)

    def own_over(i):
        return send(r.own.at[i, 0], r.own.at[i, 0], r.own_send.at[i], r.own_recv.at[i], me, buddy)

    def to_mate(i, t):
        return send(
            r.own.at[i, t], r.mate.at[i, t], r.mate_send.at[i], r.mate_recv.at[t, i],
            partner, buddy if t == 0 else leaf,
        )

    def to_leader(i):
        return send(r.pair.at[i], r.pre.at[i], r.pre_send.at[i], r.pre_recv.at[i], at(1))

    def side_over(i):
        return send(r.base.at[i], r.side.at[i], r.side_send.at[i], r.side_recv.at[i], partner)

    def swap_over(i):
        return send(r.swap.at[i], r.swap_in.at[i], r.swap_send.at[i], r.swap_recv.at[i], partner)

    def hand(i):
        return send(
            r.ready.at[i], r.slots.at[i, pl.ds(1, 2)], r.hand_send.at[i], r.hand_recv.at[i],
            me, buddy,
        )

    def chain_one(i):
        return send(r.out.at[i], r.seen.at[i], r.chain_send1.at[i], r.chain_recv.at[i], at(1))

    def chain_two(i):
        return send(r.out.at[i], r.seen.at[i], r.chain_send2.at[i], r.chain_recv.at[i], at(2))

    def root_to(i, dz, sem, side):
        return send(r.root.at[i], r.root.at[i], sem.at[i], r.root_recv.at[i], at(dz), side)

    root_dz = jnp.where(z <= ROOT_UP, 1, -2)
    root_more = (z > ROOT_UP + 2) | ((z > 0) & (z < ROOT_UP))

    def root_on(i):
        return root_to(i, root_dz, r.root_send, leaf)

    def root_low(i):
        return root_to(i, 1, r.root_send, buddy)

    def root_high(i, dz):
        return root_to(i, dz, r.root_send1 if dz == -1 else r.root_send2, buddy)

    def root_stay(i):
        return send(r.root.at[i], r.root.at[i], r.root_send3.at[i], r.root_recv.at[i], me, buddy)

    def root_over(i):
        return send(
            r.root.at[i, 1], r.slots.at[i, 0], r.over_send.at[i], r.over_recv.at[i], me, buddy
        )

    def give(i):
        return send(
            r.grads.at[i, pl.ds(0, 3)], r.given.at[i], r.give_send.at[i], r.give_recv.at[i],
            me, buddy,
        )

    def take(i):
        return send(r.taken.at[i], r.taken.at[i], r.take_send.at[i], r.take_recv.at[i], me, buddy)

    def net_over(i):
        return send(r.net.at[i], r.net_in.at[i], r.net_send.at[i], r.net_recv.at[i], at(-1))

    def back_one(i):
        return send(r.back_out.at[i], r.back.at[i], r.back_send1.at[i], r.back_recv.at[i], at(-1))

    def back_two(i):
        return send(r.back_out.at[i], r.back.at[i], r.back_send2.at[i], r.back_recv.at[i], at(-2))

    def zero_over(i):
        return send(
            r.grads.at[i, 0], r.zero.at[i], r.zero_send.at[i], r.zero_recv.at[i], me, buddy
        )

    def sum_on(i):
        return send(r.root_out.at[i], r.root_in.at[i], r.sum_send.at[i], r.sum_recv.at[i], at(2))

    def sum_last(i):
        return send(r.root_out.at[i], r.root_last.at[i], r.sum_send.at[i], r.sum_recv2.at[i], at(1))

    def sum_home(i):
        return send(r.rooted.at[i, 1], r.ra.at[i], r.ra_send.at[i], r.ra_recv.at[i], me, buddy)

    def sum_mate(i, t):
        return send(
            r.rooted.at[i, t], r.rb.at[i], r.rb_send.at[t, i], r.rb_recv.at[i],
            partner, leaf if t == 0 else buddy,
        )

    def x_over(i, t):
        return send(
            r.to_x.at[i, t], r.from_x.at[i], r.x_send.at[t, i], r.x_recv.at[i],
            partner, buddy if t == 0 else leaf,
        )

    def share(t):
        @pl.loop(0, CHUNKS)
        def _(i):
            to_mate(i, t).start()

    def store_results():
        for h in range(KEY_HEADS):
            for k, ref in enumerate((grad_keys, grad_values)):
                first = (h * 2 + k) * PARTS
                ref[:, h * WIDTH : (h + 1) * WIDTH] = (
                    r.total[first : first + PARTS].reshape(ROWS, WIDTH).astype(jnp.bfloat16)
                )
        for h in range(KEY_HEADS):
            a_out(h).wait()
            z_out(h).wait()

    def compute(h):
        q_in(h).wait()
        g_in(h).wait()
        attend(h, c, r)
        a_out(h).start()
        z_out(h).start()

    @pl.when(ends)
    def _():
        path_over().start()

        @pl.loop(0, CHUNKS)
        def _(i):
            own_over(i).start()

        share(0)

    @pl.when(relay)
    def _():
        share(1)

    prepare(depth_in(paths[...], me), assistant, r)

    @pl.when(relay)
    def _():
        path_over().wait_recv()

    deep = [
        [depth_in(r.pathv[t], b) for b in (z * 2 - 2, z * 2 - 1, z * 2, z * 2 + 1, z * 2 + 2, z * 2 + 3)]
        for t in range(2)
    ]

    def first_last(i, t):
        mine, theirs = r.own[i, t], r.mate[i, t]
        return lax.select(y == 0, mine, theirs), lax.select(y == 0, theirs, mine)

    def pairs(h):
        @pl.loop(0, PER_HEAD)
        def _(n):
            i = h * PER_HEAD + n
            own_over(i).wait_recv()
            for t in range(2):
                to_mate(i, t).wait_recv()

            @pl.when(even)
            def _():
                for t in range(2):
                    block0, block1 = first_last(i, t)
                    r.pair[i, t] = lax.select(deep[t][3] == lane, block1, block0)
                to_leader(i).start()

            @pl.when(z < 2)
            def _():
                r.seen[i] = r.own[i]

            @pl.when(z == 0)
            def _():
                for t in range(2):
                    r.root[i, t] = first_last(i, t)[0]
                for dz in (-1, -2):
                    root_high(i, dz).start()

    def ahead(h):
        @pl.loop(0, PER_HEAD)
        def _(n):
            i = h * PER_HEAD + n

            @pl.when(odd)
            def _():
                to_leader(i).wait_recv()

            @pl.when(z > 1)
            def _():
                chain_one(i).wait_recv()

            @pl.when(odd)
            def _():
                for t in range(2):
                    d_a, d_b, d_0, d_1 = deep[t][:4]
                    block0, block1 = first_last(i, t)
                    mid = lax.select((d_a == lane) | (d_b == lane), r.pre[i, t], r.seen[i, t])
                    r.out[i, t] = lax.select(
                        d_1 == lane, block1, lax.select(d_0 == lane, block0, mid)
                    )
                    r.base[i, t] = mid

            @pl.when(odd & (z < NZ - 2))
            def _():
                chain_two(i).start()

            @pl.when(odd & (z < NZ - 1))
            def _():
                chain_one(i).start()

            @pl.when(even)
            def _():
                r.base[i] = r.seen[i]

            side_over(i).start()

    def place_slots(h):
        @pl.loop(0, PER_HEAD)
        def _(n):
            i = h * PER_HEAD + n
            side_over(i).wait_recv()
            for t, ref, shift in ((0, r.ready, 1), (1, r.slots, 0)):
                for slot, at_z in ((lane, r.base), (far_lane, r.side)):
                    ref[i, slot - shift] = lax.select(
                        (deep[t][2] == slot) & (y == 1), r.mate[i, t], at_z[i, t]
                    )
            hand(i).start()

    def roots():
        @pl.loop(0, CHUNKS)
        def _(i):
            root_on(i).wait_recv()

            @pl.when(root_more)
            def _():
                root_on(i).start()

            root_over(i).start()
            r.slots[i, 0] = r.root[i, 0]

    late = (y == 1).astype(jnp.float32)
    early = 1.0 - late

    def keep(t, n):
        return (deep[t][n] != lane).astype(jnp.float32)

    def both_grads(i, t):
        mine = (r.given, r.grads)[t][i, lane]
        theirs = r.swap_in[i, t].astype(jnp.float32)
        return early * mine + late * theirs, late * mine + early * theirs

    def swaps(h):
        @pl.loop(0, PER_HEAD)
        def _(n):
            i = h * PER_HEAD + n
            give(i).wait_recv()
            for t, grad in enumerate((r.given, r.grads)):
                r.swap[i, t] = grad[i, far_lane].astype(jnp.bfloat16)
            swap_over(i).start()

    def nets(h):
        @pl.loop(0, PER_HEAD)
        def _(n):
            i = h * PER_HEAD + n
            swap_over(i).wait_recv()

            @pl.when(odd)
            def _():
                for t in range(2):
                    g0, g1 = both_grads(i, t)
                    r.net[i, t] = (keep(t, 2) * g1 + g0).astype(jnp.bfloat16)
                net_over(i).start()

    def sums():
        starts = (z == 1) | (z == 2)

        @pl.loop(0, CHUNKS)
        def _(i):
            zero_over(i).wait_recv()
            mine = (r.grads[i, 0], r.zero[i])

            @pl.when(starts)
            def _():
                for t in range(2):
                    r.root_out[i, t] = mine[t].astype(jnp.bfloat16)

            @pl.when(jnp.logical_not(starts))
            def _():
                sum_on(i).wait_recv()

            @pl.when(z > 2)
            def _():
                for t in range(2):
                    r.root_out[i, t] = (
                        mine[t] + r.root_in[i, t].astype(jnp.float32)
                    ).astype(jnp.bfloat16)

            @pl.when((z > 0) & (z < NZ - 1))
            def _():
                sum_on(i).start()

            @pl.when(z == NZ - 1)
            def _():
                sum_last(i).start()

            @pl.when(z == 0)
            def _():
                sum_last(i).wait_recv()
                for t in range(2):
                    r.rooted[i, t] = (
                        mine[t]
                        + r.root_in[i, t].astype(jnp.float32)
                        + r.root_last[i, t].astype(jnp.float32)
                    )

            @pl.when(me == 0)
            def _():
                sum_home(i).start()

            @pl.when(me == 1)
            def _():
                for t in range(2):
                    sum_mate(i, t).start()

    def backward(h):
        @pl.loop(0, PER_HEAD)
        def _(n):
            i = h * PER_HEAD + n

            @pl.when(z >= NZ - 2)
            def _():
                r.back[i] = jnp.zeros((2, CHUNK, WIDTH), jnp.bfloat16)

            @pl.when(z < NZ - 2)
            def _():
                back_one(i).wait_recv()

            @pl.when(even)
            def _():
                net_over(i).wait_recv()

            use_net = even.astype(jnp.float32)
            kept = []
            for t in range(2):
                k0, k1 = keep(t, 2), keep(t, 3)
                g0, g1 = both_grads(i, t)
                factor = use_net * (keep(t, 4) * keep(t, 5)) + (1.0 - use_net)
                before = factor * r.back[i, t].astype(jnp.float32)
                before = before + r.net_in[i, t].astype(jnp.float32)
                after = k1 * before + g1
                r.back_out[i, t] = (k0 * after + g0).astype(jnp.bfloat16)
                kept.append(((1.0 - k0) * after, (1.0 - k1) * before))

            @pl.when(even & (z > 0))
            def _():
                back_two(i).start()
                back_one(i).start()

            for t in range(2):
                taken0, taken1 = kept[t]
                r.to_x[i, t] = (early * taken1 + late * taken0).astype(jnp.bfloat16)
                x_over(i, t).start()
                mine = early * taken0 + late * taken1
                if t == 0:
                    r.taken[i] = mine
                    take(i).start()
                else:
                    r.total[i] = r.grads[i, 3] + mine

    @pl.when(odd)
    def _():
        r.net_in[...] = jnp.zeros_like(r.net_in)

    @pl.when(relay)
    def _():
        @pl.when(z > 1)
        def _():
            @pl.loop(0, KEY_HEADS)
            def _(h):
                pairs(h)

        @pl.when(lower)
        def _():
            @pl.loop(0, KEY_HEADS)
            def _(h):
                @pl.when(z < 2)
                def _():
                    pairs(h)

                ahead(h)

        @pl.when(z == 0)
        def _():
            @pl.loop(0, CHUNKS)
            def _(i):
                root_low(i).start()
                root_stay(i).start()
                r.slots[i, 0] = r.root[i, 1]

        @pl.when(lower)
        def _():
            @pl.loop(0, KEY_HEADS)
            def _(h):
                place_slots(h)

        @pl.when(upper)
        def _():
            ahead(0)

    @pl.when(ends)
    def _():
        path_over().wait_send()

        @pl.when(z > 0)
        def _():
            roots()

        @pl.when(z == 0)
        def _():
            @pl.loop(0, CHUNKS)
            def _(i):
                root_on(i).wait_recv()
                r.slots[i, 0] = r.root[i, 0]

    lag = jnp.where(z >= 12, jnp.minimum(NZ - z, 3), KEY_HEADS)

    @pl.loop(0, 2 * KEY_HEADS)
    def _(s):
        @pl.when(relay)
        def _():
            @pl.when((s >= 1) & (s <= KEY_HEADS))
            def _():
                swaps(s - 1)

            @pl.when(upper & (s < KEY_HEADS - 1))
            def _():
                ahead(s + 1)

            @pl.when(upper & (s < KEY_HEADS))
            def _():
                place_slots(s)

            @pl.when((s >= 1) & (s <= KEY_HEADS))
            def _():
                nets(s - 1)

            @pl.when((s >= lag) & (s < lag + KEY_HEADS))
            def _():
                backward(s - lag)

        @pl.when(s < KEY_HEADS)
        def _():
            @pl.when(ends)
            def _():
                @pl.loop(0, PER_HEAD)
                def _(n):
                    hand(s * PER_HEAD + n).wait_recv()

            @pl.when(relay & (z > 0))
            def _():
                @pl.loop(0, PER_HEAD)
                def _(n):
                    root_over(s * PER_HEAD + n).wait_recv()

            compute(s)

            @pl.when(relay)
            def _():
                @pl.loop(0, PER_HEAD)
                def _(n):
                    zero_over(s * PER_HEAD + n).start()

            @pl.when(ends)
            def _():
                @pl.loop(0, PER_HEAD)
                def _(n):
                    give(s * PER_HEAD + n).start()

    @pl.when(relay)
    def _():
        @pl.loop(0, CHUNKS)
        def _(i):
            x_over(i, 1).wait_recv()
            r.total[i] += r.from_x[i].astype(jnp.float32)

            @pl.when(me == 0)
            def _():
                sum_home(i).wait_recv()
                sum_mate(i, 1).wait_recv()
                r.total[i] += r.ra[i] + r.rb[i]

    @pl.when(ends)
    def _():
        sums()

        @pl.loop(0, CHUNKS)
        def _(i):
            take(i).wait_recv()
            x_over(i, 0).wait_recv()
            r.total[i] = r.grads[i, 3] + (r.taken[i] + r.from_x[i].astype(jnp.float32))

            @pl.when(me == 0)
            def _():
                sum_mate(i, 0).wait_recv()
                r.total[i] += r.rooted[i, 0] + r.rb[i]

    store_results()

    @pl.when(ends)
    def _():
        @pl.loop(0, CHUNKS)
        def _(i):
            to_mate(i, 0).wait_send()
            own_over(i).wait_send()
            give(i).wait_send()

            @pl.when(z > 0)
            def _():
                root_over(i).wait_send()
                sum_on(i).wait_send()

            @pl.when(root_more)
            def _():
                root_on(i).wait_send()

            @pl.when(me == 0)
            def _():
                sum_home(i).wait_send()

            @pl.when(me == 1)
            def _():
                for t in range(2):
                    sum_mate(i, t).wait_send()

    @pl.when(relay)
    def _():
        @pl.loop(0, CHUNKS)
        def _(i):
            to_mate(i, 1).wait_send()
            side_over(i).wait_send()
            swap_over(i).wait_send()
            hand(i).wait_send()
            take(i).wait_send()
            for t in range(2):
                x_over(i, t).wait_send()

            zero_over(i).wait_send()

            @pl.when(z == 0)
            def _():
                root_low(i).wait_send()
                root_stay(i).wait_send()
                for dz in (-1, -2):
                    root_high(i, dz).wait_send()

            @pl.when(even)
            def _():
                to_leader(i).wait_send()

            @pl.when(odd & (z < NZ - 1))
            def _():
                chain_one(i).wait_send()

            @pl.when(odd & (z < NZ - 2))
            def _():
                chain_two(i).wait_send()

            @pl.when(odd)
            def _():
                net_over(i).wait_send()

            @pl.when(even & (z > 0))
            def _():
                back_one(i).wait_send()
                back_two(i).wait_send()


def on_device(queries, keys, values, grad_out, block_path, assistant):
    paths = block_path.T
    extra = scratch(paths.shape)
    vmem = pl.BlockSpec(memory_space=pltpu.VMEM)
    anywhere = pl.BlockSpec(memory_space=pl.ANY)
    wide = jax.ShapeDtypeStruct(queries.shape, jnp.bfloat16)
    small = jax.ShapeDtypeStruct(keys.shape, jnp.bfloat16)
    return pl.pallas_call(
        functools.partial(step_kernel, tuple(extra)),
        out_shape=(wide, wide, small, small),
        in_specs=[vmem] * 4 + [anywhere] * 2,
        out_specs=(anywhere, anywhere, vmem, vmem),
        scratch_shapes=list(extra.values()),
        compiler_params=pltpu.CompilerParams(collective_id=0, has_side_effects=True),
        name="step",
    )(paths, assistant.reshape(1, ROWS), keys, values, queries, grad_out)


def solution(mesh):
    rows = P(("leaf", "ctx"), None)
    in_specs = (rows, rows, rows, rows, P("leaf", None), P(("leaf", "ctx")))
    return jax.shard_map(
        on_device, mesh=mesh, in_specs=in_specs, out_specs=(rows,) * 4, check_vma=False
    )
```

```python
import functools
import math
import types

import jax
import jax.numpy as jnp
from jax import lax
from jax.experimental import pallas as pl
from jax.experimental.pallas import tpu as pltpu
from jax.sharding import PartitionSpec as P

KEY_HEADS = 4
WIDTH = 128
GROUP = 8
ROWS = 128
NZ = 16
UPPER = 10
ROOT_UP = 4
SUM_DOWN = 7
PARTS = 2
CUTS = 4
CHUNK = ROWS // PARTS
PER_HEAD = 2 * PARTS
CHUNKS = KEY_HEADS * PER_HEAD
SCALE = 1.0 / math.sqrt(WIDTH)
EXP2_SCALE = SCALE * math.log2(math.e)
MASKED = -1e30


def place():
    me = lax.axis_index("ctx")
    return me, me // 2, lax.rem(me, 2)


def depth_in(paths, block):
    at = lax.broadcasted_iota(jnp.int32, paths.shape, 1) == block
    return jnp.sum((at & (paths >= 0)).astype(jnp.int32)) - 1


def send(src, dst, send_sem, recv_sem, ctx, leaf=None):
    device = {"ctx": ctx} if leaf is None else {"leaf": leaf, "ctx": ctx}
    return pltpu.make_async_remote_copy(
        src_ref=src,
        dst_ref=dst,
        send_sem=send_sem,
        recv_sem=recv_sem,
        device_id=device,
        device_id_type=pl.DeviceIdType.MESH,
    )


def greet(peers):
    barrier = pltpu.get_barrier_semaphore()
    for peer, leaf in peers:
        pl.semaphore_signal(
            barrier,
            inc=1,
            device_id={"leaf": leaf, "ctx": peer},
            device_id_type=pl.DeviceIdType.MESH,
        )
    pl.semaphore_wait(barrier, len(peers))


def scratch(trees):
    def room(*lead, dtype=jnp.bfloat16):
        return pltpu.VMEM((CHUNKS, *lead, CHUNK, WIDTH), dtype)

    full = jnp.float32
    wide = pltpu.VMEM((KEY_HEADS, ROWS, GROUP * WIDTH), jnp.bfloat16)
    sem = pltpu.SemaphoreType.DMA
    one = sem((CHUNKS,))
    two = sem((2, CHUNKS))
    heads = sem((KEY_HEADS,))
    return dict(
        qv=wide, gv=wide, av=wide, zv=wide,
        bias=pltpu.VMEM((4 * ROWS, 2 * ROWS), full),
        live=pltpu.VMEM((ROWS, ROWS), jnp.bfloat16),
        d_all=pltpu.VMEM((4 * ROWS, GROUP * ROWS), jnp.bfloat16),
        w_all=pltpu.VMEM((4 * ROWS, GROUP * ROWS), jnp.bfloat16),
        q_all=pltpu.VMEM((GROUP * ROWS, WIDTH), jnp.bfloat16),
        g_all=pltpu.VMEM((GROUP * ROWS, WIDTH), jnp.bfloat16),
        pathv=pltpu.VMEM((2, *trees), jnp.int32),
        own=room(2), mate=room(2), pair=room(2), pre=room(2), root=room(2),
        seen=room(2), out=room(2), base=room(2), side=room(2),
        ready=room(2), slots=room(3),
        grads=room(4, dtype=full), given=room(3, dtype=full), swap=room(2), swap_in=room(2),
        net=room(2), net_in=room(2), back=room(2), back_out=room(2), total=room(dtype=full),
        root_in=room(2), root_end=room(2), root_last=room(2), root_out=room(2),
        rooted=room(2, dtype=full), ra=room(dtype=full), rb=room(dtype=full), zero=room(dtype=full), to_x=room(2), from_x=room(), taken=room(dtype=full),
        q_sem=heads, g_sem=heads, a_sem=heads, z_sem=heads,
        path_send=sem, path_recv=sem,
        own_send=one, own_recv=one, mate_send=one, mate_recv=two,
        pre_send=one, pre_recv=one, side_send=one, side_recv=one, swap_send=one, swap_recv=one,
        root_send=one, root_send1=one, root_send2=one, root_send3=one, over_send=one, over_recv=one,
        zero_send=one, zero_recv=one, ra_send=one, ra_recv=one, rb_send=two, rb_recv=one, root_recv=one,
        chain_send1=one, chain_send2=one, chain_recv=one, hand_send=one, hand_recv=one,
        give_send=one, give_recv=one, take_send=one, take_recv=one,
        net_send=one, net_recv=one, back_send1=one, back_send2=one, back_recv=one,
        sum_send=one, sum_recv=one, sum_recv1=one, sum_recv2=one, x_send=two, x_recv=one,
    )


def attend(h, c, r):
    first = h * PER_HEAD

    def block(at, offset, *where):
        return at[(pl.ds(first + offset, PARTS), *where)].reshape(ROWS, WIDTH)

    k4 = jnp.concatenate([block(r.slots, 0, e) for e in range(3)] + [block(r.own, 0, c)], 0)
    v4 = jnp.concatenate([block(r.slots, PARTS, e) for e in range(3)] + [block(r.own, PARTS, c)], 0)
    k4t = k4.T
    v4t = v4.T
    dims = (((1,), (1,)), ((), ()))
    for pair in range(GROUP // 2):
        at = [slice((2 * pair + j) * WIDTH, (2 * pair + j + 1) * WIDTH) for j in range(2)]
        q2 = jnp.concatenate([r.qv[h, :, s] for s in at], 0)
        g2 = jnp.concatenate([r.gv[h, :, s] * r.live[...] for s in at], 0)
        s = lax.dot_general(k4, q2, dims, preferred_element_type=jnp.float32) + r.bias[...]
        top = jnp.max(s, axis=0, keepdims=True)
        p = jnp.exp2((s - top) * EXP2_SCALE)
        w = p * (1.0 / jnp.sum(p, axis=0, keepdims=True))
        wb = w.astype(jnp.bfloat16)
        out_t = jnp.dot(v4t, wb, preferred_element_type=jnp.float32)
        dp = lax.dot_general(v4, g2, dims, preferred_element_type=jnp.float32)
        out_t = out_t.astype(jnp.bfloat16)
        delta = jnp.sum(
            g2.T.astype(jnp.float32) * out_t.astype(jnp.float32), axis=0, keepdims=True
        )
        ds = (w * (dp - delta)).astype(jnp.bfloat16)
        gq_t = jnp.dot(k4t, ds, preferred_element_type=jnp.float32) * SCALE
        out = out_t.T
        gq = gq_t.astype(jnp.bfloat16).T
        for j in range(2):
            r.av[h, :, at[j]] = out[j * ROWS : (j + 1) * ROWS]
            r.zv[h, :, at[j]] = gq[j * ROWS : (j + 1) * ROWS]
        here = slice(pair * 2 * ROWS, (pair + 1) * 2 * ROWS)
        r.d_all[:, here] = ds
        r.w_all[:, here] = wb
        r.q_all[here] = q2
        r.g_all[here] = g2
    dk = jnp.dot(r.d_all[...], r.q_all[...], preferred_element_type=jnp.float32) * SCALE
    dv = jnp.dot(r.w_all[...], r.g_all[...], preferred_element_type=jnp.float32)
    for t, d in enumerate((dk, dv)):
        for e in range(4):
            r.grads[pl.ds(first + t * PARTS, PARTS), e] = d[
                e * ROWS : (e + 1) * ROWS
            ].reshape(PARTS, CHUNK, WIDTH)


def prepare(depth, assistant, r):
    cols = 2 * ROWS
    for e in range(3):
        r.bias[e * ROWS : (e + 1) * ROWS] = jnp.full(
            (ROWS, cols), jnp.where(e < depth, 0.0, MASKED), jnp.float32
        )
    key_at = lax.broadcasted_iota(jnp.int32, (ROWS, cols), 0)
    row_at = lax.broadcasted_iota(jnp.int32, (ROWS, cols), 1)
    row_at = jnp.where(row_at >= ROWS, row_at - ROWS, row_at)
    r.bias[3 * ROWS :] = jnp.where(key_at <= row_at, 0.0, MASKED)
    i = lax.broadcasted_iota(jnp.int32, (ROWS, ROWS), 0)
    j = lax.broadcasted_iota(jnp.int32, (ROWS, ROWS), 1)
    spread = jnp.where(i == j, assistant[...].astype(jnp.float32), 0.0)
    r.live[...] = jnp.broadcast_to(
        jnp.sum(spread, axis=1, keepdims=True), (ROWS, ROWS)
    ).astype(jnp.bfloat16)


def step_kernel(names, paths, assistant, keys, values, queries, grad_out, *refs):
    attention, grad_queries, grad_keys, grad_values = refs[:4]
    r = types.SimpleNamespace(**dict(zip(names, refs[4:])))
    me, z, y = place()
    leaf = lax.axis_index("leaf")
    c = lax.rem(leaf, 2)
    relay = c == 1
    ends = jnp.logical_not(relay)
    buddy = jnp.where(relay, leaf - 1, leaf + 1)
    odd = lax.rem(z, 2) == 1
    even = jnp.logical_not(odd)
    upper = z >= UPPER
    lower = jnp.logical_not(upper)

    def at(dz, side=None):
        return lax.rem(z + dz + NZ, NZ) * 2 + (y if side is None else side)

    other = 1 - y
    partner = at(0, other)
    lane = 1 + y
    far_lane = 2 - y

    def column(h):
        return pl.ds(pl.multiple_of(h * GROUP * WIDTH, GROUP * WIDTH), GROUP * WIDTH)

    def q_in(h):
        return pltpu.make_async_copy(queries.at[:, column(h)], r.qv.at[h], r.q_sem.at[h])

    def g_in(h):
        return pltpu.make_async_copy(grad_out.at[:, column(h)], r.gv.at[h], r.g_sem.at[h])

    def a_out(h):
        return pltpu.make_async_copy(r.av.at[h], attention.at[:, column(h)], r.a_sem.at[h])

    def z_out(h):
        return pltpu.make_async_copy(r.zv.at[h], grad_queries.at[:, column(h)], r.z_sem.at[h])

    for h in range(KEY_HEADS):
        q_in(h).start()
        g_in(h).start()
    for h in range(KEY_HEADS):
        for k, ref in enumerate((keys, values)):
            first = (h * 2 + k) * PARTS
            r.own[first : first + PARTS, c] = ref[:, h * WIDTH : (h + 1) * WIDTH].reshape(
                PARTS, CHUNK, WIDTH
            )
    r.pathv[1] = paths[...]

    @pl.when(ends)
    def _():
        r.pathv[0] = paths[...]


    greet(
        (
            (at(1), leaf), (at(-1), leaf), (at(2), leaf), (at(-2), leaf), (partner, leaf),
            (me, buddy), (partner, buddy), (at(1), buddy), (at(-1), buddy),
            (at(2), buddy), (at(-2), buddy),
        )
    )

    def path_over():
        return send(r.pathv.at[0], r.pathv.at[0], r.path_send, r.path_recv, me, buddy)

    def own_over(i):
        return send(r.own.at[i, 0], r.own.at[i, 0], r.own_send.at[i], r.own_recv.at[i], me, buddy)

    def to_mate(i, t):
        return send(
            r.own.at[i, t], r.mate.at[i, t], r.mate_send.at[i], r.mate_recv.at[t, i],
            partner, buddy if t == 0 else leaf,
        )

    def to_leader(i):
        return send(r.pair.at[i], r.pre.at[i], r.pre_send.at[i], r.pre_recv.at[i], at(1))

    def side_over(i):
        return send(r.base.at[i], r.side.at[i], r.side_send.at[i], r.side_recv.at[i], partner)

    def swap_over(i):
        return send(r.swap.at[i], r.swap_in.at[i], r.swap_send.at[i], r.swap_recv.at[i], partner)

    def hand(i):
        return send(
            r.ready.at[i], r.slots.at[i, pl.ds(1, 2)], r.hand_send.at[i], r.hand_recv.at[i],
            me, buddy,
        )

    def chain_one(i):
        return send(r.out.at[i], r.seen.at[i], r.chain_send1.at[i], r.chain_recv.at[i], at(1))

    def chain_two(i):
        return send(r.out.at[i], r.seen.at[i], r.chain_send2.at[i], r.chain_recv.at[i], at(2))

    def root_to(i, dz, sem, side):
        return send(r.root.at[i], r.root.at[i], sem.at[i], r.root_recv.at[i], at(dz), side)

    root_dz = jnp.where(z <= ROOT_UP, 1, -2)
    root_more = (z > ROOT_UP + 2) | ((z > 0) & (z < ROOT_UP))

    def root_on(i):
        return root_to(i, root_dz, r.root_send, leaf)

    def root_low(i):
        return root_to(i, 1, r.root_send, buddy)

    def root_high(i, dz):
        return root_to(i, dz, r.root_send1 if dz == -1 else r.root_send2, buddy)

    def root_stay(i):
        return send(r.root.at[i], r.root.at[i], r.root_send3.at[i], r.root_recv.at[i], me, buddy)

    def root_over(i):
        return send(
            r.root.at[i, 1], r.slots.at[i, 0], r.over_send.at[i], r.over_recv.at[i], me, buddy
        )

    def give(i):
        return send(
            r.grads.at[i, pl.ds(0, 3)], r.given.at[i], r.give_send.at[i], r.give_recv.at[i],
            me, buddy,
        )

    def take(i):
        return send(r.taken.at[i], r.taken.at[i], r.take_send.at[i], r.take_recv.at[i], me, buddy)

    def net_over(i):
        return send(r.net.at[i], r.net_in.at[i], r.net_send.at[i], r.net_recv.at[i], at(-1))

    def back_one(i):
        return send(r.back_out.at[i], r.back.at[i], r.back_send1.at[i], r.back_recv.at[i], at(-1))

    def back_two(i):
        return send(r.back_out.at[i], r.back.at[i], r.back_send2.at[i], r.back_recv.at[i], at(-2))

    def zero_over(i):
        return send(
            r.grads.at[i, 0], r.zero.at[i], r.zero_send.at[i], r.zero_recv.at[i], me, buddy
        )

    def sum_on(i):
        return send(
            r.root_out.at[i], r.root_in.at[i], r.sum_send.at[i], r.sum_recv.at[i],
            at(jnp.where(z <= SUM_DOWN, -1, 2)),
        )

    def sum_end(i):
        return send(r.root_out.at[i], r.root_end.at[i], r.sum_send.at[i], r.sum_recv1.at[i], at(2))

    def sum_last(i):
        return send(r.root_out.at[i], r.root_last.at[i], r.sum_send.at[i], r.sum_recv2.at[i], at(1))

    def sum_home(i):
        return send(r.rooted.at[i, 1], r.ra.at[i], r.ra_send.at[i], r.ra_recv.at[i], me, buddy)

    def sum_mate(i, t):
        return send(
            r.rooted.at[i, t], r.rb.at[i], r.rb_send.at[t, i], r.rb_recv.at[i],
            partner, leaf if t == 0 else buddy,
        )

    def x_over(i, t):
        return send(
            r.to_x.at[i, t], r.from_x.at[i], r.x_send.at[t, i], r.x_recv.at[i],
            partner, buddy if t == 0 else leaf,
        )

    def share(t):
        @pl.loop(0, CHUNKS)
        def _(i):
            to_mate(i, t).start()

    def store_results():
        for h in range(KEY_HEADS):
            for k, ref in enumerate((grad_keys, grad_values)):
                first = (h * 2 + k) * PARTS
                ref[:, h * WIDTH : (h + 1) * WIDTH] = (
                    r.total[first : first + PARTS].reshape(ROWS, WIDTH).astype(jnp.bfloat16)
                )
        for h in range(KEY_HEADS):
            a_out(h).wait()
            z_out(h).wait()

    def compute(h):
        q_in(h).wait()
        g_in(h).wait()
        attend(h, c, r)
        a_out(h).start()
        z_out(h).start()

    @pl.when(ends)
    def _():
        path_over().start()

        @pl.loop(0, CHUNKS)
        def _(i):
            own_over(i).start()

        share(0)

    @pl.when(relay)
    def _():
        share(1)

    prepare(depth_in(paths[...], me), assistant, r)

    @pl.when(relay)
    def _():
        path_over().wait_recv()

    deep = [
        [depth_in(r.pathv[t], b) for b in (z * 2 - 2, z * 2 - 1, z * 2, z * 2 + 1, z * 2 + 2, z * 2 + 3)]
        for t in range(2)
    ]

    def first_last(i, t):
        mine, theirs = r.own[i, t], r.mate[i, t]
        return lax.select(y == 0, mine, theirs), lax.select(y == 0, theirs, mine)

    def pairs(h):
        @pl.loop(0, PER_HEAD)
        def _(n):
            i = h * PER_HEAD + n
            own_over(i).wait_recv()
            for t in range(2):
                to_mate(i, t).wait_recv()

            @pl.when(even)
            def _():
                for t in range(2):
                    block0, block1 = first_last(i, t)
                    r.pair[i, t] = lax.select(deep[t][3] == lane, block1, block0)
                to_leader(i).start()

            @pl.when(z < 2)
            def _():
                r.seen[i] = r.own[i]

            @pl.when(z == 0)
            def _():
                for t in range(2):
                    r.root[i, t] = first_last(i, t)[0]
                for dz in (-1, -2):
                    root_high(i, dz).start()

    def ahead(h):
        @pl.loop(0, PER_HEAD)
        def _(n):
            i = h * PER_HEAD + n

            @pl.when(odd)
            def _():
                to_leader(i).wait_recv()

            @pl.when(z > 1)
            def _():
                chain_one(i).wait_recv()

            @pl.when(odd)
            def _():
                for t in range(2):
                    d_a, d_b, d_0, d_1 = deep[t][:4]
                    block0, block1 = first_last(i, t)
                    mid = lax.select((d_a == lane) | (d_b == lane), r.pre[i, t], r.seen[i, t])
                    r.out[i, t] = lax.select(
                        d_1 == lane, block1, lax.select(d_0 == lane, block0, mid)
                    )
                    r.base[i, t] = mid

            @pl.when(odd & (z < NZ - 2))
            def _():
                chain_two(i).start()

            @pl.when(odd & (z < NZ - 1))
            def _():
                chain_one(i).start()

            @pl.when(even)
            def _():
                r.base[i] = r.seen[i]

            side_over(i).start()

    def place_slots(h):
        @pl.loop(0, PER_HEAD)
        def _(n):
            i = h * PER_HEAD + n
            side_over(i).wait_recv()
            for t, ref, shift in ((0, r.ready, 1), (1, r.slots, 0)):
                for slot, at_z in ((lane, r.base), (far_lane, r.side)):
                    ref[i, slot - shift] = lax.select(
                        (deep[t][2] == slot) & (y == 1), r.mate[i, t], at_z[i, t]
                    )
            hand(i).start()

    def roots():
        @pl.loop(0, CHUNKS)
        def _(i):
            root_on(i).wait_recv()

            @pl.when(root_more)
            def _():
                root_on(i).start()

            root_over(i).start()
            r.slots[i, 0] = r.root[i, 0]

    late = (y == 1).astype(jnp.float32)
    early = 1.0 - late

    def keep(t, n):
        return (deep[t][n] != lane).astype(jnp.float32)

    def both_grads(i, t):
        mine = (r.given, r.grads)[t][i, lane]
        theirs = r.swap_in[i, t].astype(jnp.float32)
        return early * mine + late * theirs, late * mine + early * theirs

    def swaps(h):
        @pl.loop(0, PER_HEAD)
        def _(n):
            i = h * PER_HEAD + n
            give(i).wait_recv()
            for t, grad in enumerate((r.given, r.grads)):
                r.swap[i, t] = grad[i, far_lane].astype(jnp.bfloat16)
            swap_over(i).start()

    def nets(h):
        @pl.loop(0, PER_HEAD)
        def _(n):
            i = h * PER_HEAD + n
            swap_over(i).wait_recv()

            @pl.when(odd)
            def _():
                for t in range(2):
                    g0, g1 = both_grads(i, t)
                    r.net[i, t] = (keep(t, 2) * g1 + g0).astype(jnp.bfloat16)
                net_over(i).start()

    def sums():
        starts = (z == SUM_DOWN) | (z == SUM_DOWN + 1) | (z == SUM_DOWN + 2)

        @pl.loop(0, CHUNKS)
        def _(i):
            zero_over(i).wait_recv()
            mine = (r.grads[i, 0], r.zero[i])

            @pl.when(starts)
            def _():
                for t in range(2):
                    r.root_out[i, t] = mine[t].astype(jnp.bfloat16)

            @pl.when(jnp.logical_not(starts))
            def _():
                sum_on(i).wait_recv()

            @pl.when(jnp.logical_not(starts) & (z > 0))
            def _():
                for t in range(2):
                    r.root_out[i, t] = (
                        mine[t] + r.root_in[i, t].astype(jnp.float32)
                    ).astype(jnp.bfloat16)

            @pl.when((z > 0) & (z < NZ - 2))
            def _():
                sum_on(i).start()

            @pl.when(z == NZ - 2)
            def _():
                sum_end(i).start()

            @pl.when(z == NZ - 1)
            def _():
                sum_last(i).start()

            @pl.when(z == 0)
            def _():
                sum_end(i).wait_recv()
                sum_last(i).wait_recv()
                for t in range(2):
                    r.rooted[i, t] = (mine[t] + r.root_in[i, t].astype(jnp.float32)) + (
                        r.root_end[i, t].astype(jnp.float32)
                        + r.root_last[i, t].astype(jnp.float32)
                    )

            @pl.when(me == 0)
            def _():
                sum_home(i).start()

            @pl.when(me == 1)
            def _():
                for t in range(2):
                    sum_mate(i, t).start()

    def backward(h):
        @pl.loop(0, PER_HEAD)
        def _(n):
            i = h * PER_HEAD + n

            @pl.when(z >= NZ - 2)
            def _():
                r.back[i] = jnp.zeros((2, CHUNK, WIDTH), jnp.bfloat16)

            @pl.when(z < NZ - 2)
            def _():
                back_one(i).wait_recv()

            @pl.when(even)
            def _():
                net_over(i).wait_recv()

            use_net = even.astype(jnp.float32)
            kept = []
            for t in range(2):
                k0, k1 = keep(t, 2), keep(t, 3)
                g0, g1 = both_grads(i, t)
                factor = use_net * (keep(t, 4) * keep(t, 5)) + (1.0 - use_net)
                before = factor * r.back[i, t].astype(jnp.float32)
                before = before + r.net_in[i, t].astype(jnp.float32)
                after = k1 * before + g1
                r.back_out[i, t] = (k0 * after + g0).astype(jnp.bfloat16)
                kept.append(((1.0 - k0) * after, (1.0 - k1) * before))

            @pl.when(even & (z > 0))
            def _():
                back_two(i).start()
                back_one(i).start()

            for t in range(2):
                taken0, taken1 = kept[t]
                r.to_x[i, t] = (early * taken1 + late * taken0).astype(jnp.bfloat16)
                x_over(i, t).start()
                mine = early * taken0 + late * taken1
                if t == 0:
                    r.taken[i] = mine
                    take(i).start()
                else:
                    r.total[i] = r.grads[i, 3] + mine

    @pl.when(odd)
    def _():
        r.net_in[...] = jnp.zeros_like(r.net_in)

    @pl.when(relay)
    def _():
        @pl.when(z > 1)
        def _():
            @pl.loop(0, KEY_HEADS)
            def _(h):
                pairs(h)

        @pl.when(lower)
        def _():
            @pl.loop(0, KEY_HEADS)
            def _(h):
                @pl.when(z < 2)
                def _():
                    pairs(h)

                ahead(h)

        @pl.when(z == 0)
        def _():
            @pl.loop(0, CHUNKS)
            def _(i):
                root_low(i).start()
                root_stay(i).start()
                r.slots[i, 0] = r.root[i, 1]

        @pl.when(lower)
        def _():
            @pl.loop(0, KEY_HEADS)
            def _(h):
                place_slots(h)

        @pl.when(upper)
        def _():
            ahead(0)

    @pl.when(ends)
    def _():
        path_over().wait_send()

        @pl.when(z > 0)
        def _():
            roots()

        @pl.when(z == 0)
        def _():
            @pl.loop(0, CHUNKS)
            def _(i):
                root_on(i).wait_recv()
                r.slots[i, 0] = r.root[i, 0]

    lag = jnp.where(z >= 12, jnp.minimum(NZ - z, 3), KEY_HEADS)

    @pl.loop(0, 2 * KEY_HEADS)
    def _(s):
        @pl.when(relay)
        def _():
            @pl.when((s >= 1) & (s <= KEY_HEADS))
            def _():
                swaps(s - 1)

            @pl.when(upper & (s < KEY_HEADS - 1))
            def _():
                ahead(s + 1)

            @pl.when(upper & (s < KEY_HEADS))
            def _():
                place_slots(s)

            @pl.when((s >= 1) & (s <= KEY_HEADS))
            def _():
                nets(s - 1)

            @pl.when((s >= lag) & (s < lag + KEY_HEADS))
            def _():
                backward(s - lag)

        @pl.when(s < KEY_HEADS)
        def _():
            @pl.when(ends)
            def _():
                @pl.loop(0, PER_HEAD)
                def _(n):
                    hand(s * PER_HEAD + n).wait_recv()

            @pl.when(relay & (z > 0))
            def _():
                @pl.loop(0, PER_HEAD)
                def _(n):
                    root_over(s * PER_HEAD + n).wait_recv()

            compute(s)

            @pl.when(relay)
            def _():
                @pl.loop(0, PER_HEAD)
                def _(n):
                    zero_over(s * PER_HEAD + n).start()

            @pl.when(ends)
            def _():
                @pl.loop(0, PER_HEAD)
                def _(n):
                    give(s * PER_HEAD + n).start()

    @pl.when(relay)
    def _():
        @pl.loop(0, CHUNKS)
        def _(i):
            x_over(i, 1).wait_recv()
            r.total[i] += r.from_x[i].astype(jnp.float32)

            @pl.when(me == 0)
            def _():
                sum_home(i).wait_recv()
                sum_mate(i, 1).wait_recv()
                r.total[i] += r.ra[i] + r.rb[i]

    @pl.when(ends)
    def _():
        sums()

        @pl.loop(0, CHUNKS)
        def _(i):
            take(i).wait_recv()
            x_over(i, 0).wait_recv()
            r.total[i] = r.grads[i, 3] + (r.taken[i] + r.from_x[i].astype(jnp.float32))

            @pl.when(me == 0)
            def _():
                sum_mate(i, 0).wait_recv()
                r.total[i] += r.rooted[i, 0] + r.rb[i]

    store_results()

    @pl.when(ends)
    def _():
        @pl.loop(0, CHUNKS)
        def _(i):
            to_mate(i, 0).wait_send()
            own_over(i).wait_send()
            give(i).wait_send()

            @pl.when(z > 0)
            def _():
                root_over(i).wait_send()
                sum_on(i).wait_send()

            @pl.when(root_more)
            def _():
                root_on(i).wait_send()

            @pl.when(me == 0)
            def _():
                sum_home(i).wait_send()

            @pl.when(me == 1)
            def _():
                for t in range(2):
                    sum_mate(i, t).wait_send()

    @pl.when(relay)
    def _():
        @pl.loop(0, CHUNKS)
        def _(i):
            to_mate(i, 1).wait_send()
            side_over(i).wait_send()
            swap_over(i).wait_send()
            hand(i).wait_send()
            take(i).wait_send()
            for t in range(2):
                x_over(i, t).wait_send()

            zero_over(i).wait_send()

            @pl.when(z == 0)
            def _():
                root_low(i).wait_send()
                root_stay(i).wait_send()
                for dz in (-1, -2):
                    root_high(i, dz).wait_send()

            @pl.when(even)
            def _():
                to_leader(i).wait_send()

            @pl.when(odd & (z < NZ - 1))
            def _():
                chain_one(i).wait_send()

            @pl.when(odd & (z < NZ - 2))
            def _():
                chain_two(i).wait_send()

            @pl.when(odd)
            def _():
                net_over(i).wait_send()

            @pl.when(even & (z > 0))
            def _():
                back_one(i).wait_send()
                back_two(i).wait_send()


def finish_kernel(cuts, *refs):
    sources, results, held = refs[:4], refs[4:8], refs[8:12]
    in_sem, out_sem = refs[12:]

    def rows(j, cut):
        size = ROWS // (CUTS if j < 2 else 1)
        return pl.ds(cut * size, size)

    loads, stores = [], []
    for n, (j, cut) in enumerate(cuts):
        at = rows(j, cut)
        loads.append(
            pltpu.make_async_copy(sources[j].at[at], held[j].at[at], in_sem.at[n])
        )
        stores.append(
            pltpu.make_async_copy(held[j].at[at], results[j].at[at], out_sem.at[n])
        )
    for load in loads:
        load.start()
    for load, store in zip(loads, stores):
        load.wait()
        store.start()
    for store in stores:
        store.wait()


def on_device(queries, keys, values, grad_out, block_path, assistant):
    paths = block_path.T
    extra = scratch(paths.shape)
    vmem = pl.BlockSpec(memory_space=pltpu.VMEM)
    anywhere = pl.BlockSpec(memory_space=pl.ANY)
    wide = jax.ShapeDtypeStruct(queries.shape, jnp.bfloat16)
    small = jax.ShapeDtypeStruct(keys.shape, jnp.bfloat16)
    results = pl.pallas_call(
        functools.partial(step_kernel, tuple(extra)),
        out_shape=(wide, wide, small, small),
        in_specs=[vmem] * 4 + [anywhere] * 2,
        out_specs=(anywhere, anywhere, vmem, vmem),
        scratch_shapes=list(extra.values()),
        compiler_params=pltpu.CompilerParams(collective_id=0, has_side_effects=True),
        name="step",
    )(paths, assistant.reshape(1, ROWS), keys, values, queries, grad_out)
    cuts = [(j, cut) for j in range(2) for cut in range(CUTS)] + [(2, 0), (3, 0)]
    return pl.pallas_call(
        functools.partial(finish_kernel, cuts),
        out_shape=(wide, wide, small, small),
        in_specs=[anywhere] * 4,
        out_specs=(anywhere,) * 4,
        scratch_shapes=[pltpu.VMEM(a.shape, a.dtype) for a in (wide, wide, small, small)]
        + [pltpu.SemaphoreType.DMA((len(cuts),))] * 2,
        name="finish",
    )(*results)


def solution(mesh):
    rows = P(("leaf", "ctx"), None)
    in_specs = (rows, rows, rows, rows, P("leaf", None), P(("leaf", "ctx")))
    return jax.shard_map(
        on_device, mesh=mesh, in_specs=in_specs, out_specs=(rows,) * 4, check_vma=False
    )
```
